16 devices in a mesh: dp: 2 (over z), tp: 8 (over y, x, core).
Axes of the slice: x: 2, y: 2, z: 2, core: 2. Of those that a mesh axis runs over, the one named last changes fastest.
Arguments:
- x: bfloat16 [64, 256, 1152], P('dp', 'tp'), parts along dimension 0
- d_out: bfloat16 [64, 256, 1152], P('dp', 'tp'), parts along dimension 0
- ln1_gain: float32 [1152], replicated
- ln1_bias: float32 [1152], replicated
- w_q: bfloat16 [1152, 16, 72], P(None, 'tp')
- b_q: bfloat16 [16, 72], P('tp')
- w_k: bfloat16 [1152, 16, 72], P(None, 'tp')
- w_v: bfloat16 [1152, 16, 72], P(None, 'tp')
- b_v: bfloat16 [16, 72], P('tp')
- w_o: bfloat16 [16, 72, 1152], P('tp')
- b_o: bfloat16 [1152], replicated
- ln2_gain: float32 [1152], replicated
- ln2_bias: float32 [1152], replicated
- w_1: bfloat16 [1152, 4304], P(None, 'tp')
- b_1: bfloat16 [4304], P('tp')
- w_2: bfloat16 [4304, 1152], P('tp')
- b_2: bfloat16 [1152], replicated
Outputs:
- output 1: bfloat16 [64, 256, 1152], P('dp', 'tp'), parts along dimension 0
- output 2: bfloat16 [64, 256, 1152], P('dp', 'tp'), parts along dimension 0
- output 3: float32 [2304], P('dp'), parts along dimension 0
- output 4: float32 [2304], P('dp'), parts along dimension 0
- output 5: bfloat16 [2304, 16, 72], P('dp', 'tp'), parts along dimension 0
- output 6: bfloat16 [32, 72], P(('dp', 'tp')), parts along dimension 0
- output 7: bfloat16 [2304, 16, 72], P('dp', 'tp'), parts along dimension 0
- output 8: bfloat16 [2304, 16, 72], P('dp', 'tp'), parts along dimension 0
- output 9: bfloat16 [32, 72], P(('dp', 'tp')), parts along dimension 0
- output 10: bfloat16 [32, 72, 1152], P(('dp', 'tp')), parts along dimension 0
- output 11: bfloat16 [2304], P('dp'), parts along dimension 0
- output 12: float32 [2304], P('dp'), parts along dimension 0
- output 13: float32 [2304], P('dp'), parts along dimension 0
- output 14: bfloat16 [2304, 4304], P('dp', 'tp'), parts along dimension 0
- output 15: bfloat16 [8608], P(('dp', 'tp')), parts along dimension 0
- output 16: bfloat16 [8608, 1152], P(('dp', 'tp')), parts along dimension 0
- output 17: bfloat16 [2304], P('dp'), parts along dimension 0
There are 2 independent parts. The reference program is written for one: setup_inputs(seed, part) draws one part's arguments, and reference() takes and returns one part's arrays. A program takes and returns all parts, laid end to end along the dimension named above; an argument that names none is the same for every part.
All inputs are finite; a program needn't handle non-finite values.
Results may differ from the reference program's by a relative error of at most 0.0189534.
Values are sent between devices in bfloat16 or wider.
A program may use at most 1 GiB of HBM per device.

```python
import math
import jax
import jax.numpy as jnp
from jax import lax

IMAGES = 32
PATCHES = 256
WIDTH = 1152
NUM_HEADS = 16
HEAD_DIM = 72
MLP_DIM = 4304
LN_EPS = 1e-6
ATT_SCALE = 1.0 / math.sqrt(HEAD_DIM)
TOKENS = IMAGES * PATCHES


def draw_normal(key, shape, scale):
    return jax.random.normal(key, shape, jnp.float32) * scale


def setup_inputs(seed: int = 0, part: int = 0) -> dict:
    part_key = jax.random.fold_in(jax.random.key(seed), part)
    act_keys = jax.random.split(part_key, 4)
    wt_keys = jax.random.split(jax.random.key(seed + 1), 15)
    act_shape = (IMAGES, PATCHES, WIDTH)
    row_scale = jnp.exp(draw_normal(act_keys[0], (IMAGES, PATCHES, 1), 0.5))
    row_shift = draw_normal(act_keys[1], (IMAGES, PATCHES, 1), 0.5)
    x = (draw_normal(act_keys[2], act_shape, 1.0) * row_scale + row_shift).astype(jnp.bfloat16)
    d_out = draw_normal(act_keys[3], act_shape, 1.0).astype(jnp.bfloat16)
    in_scale = WIDTH ** -0.5
    qk_scale = in_scale * math.sqrt(math.sqrt(math.log(PATCHES / 8.0)))
    head_w = (WIDTH, NUM_HEADS, HEAD_DIM)
    head_b = (NUM_HEADS, HEAD_DIM)
    return {
        'x': x,
        'd_out': d_out,
        'ln1_gain': 1.0 + draw_normal(wt_keys[0], (WIDTH,), 0.25),
        'ln1_bias': draw_normal(wt_keys[1], (WIDTH,), 0.3),
        'w_q': draw_normal(wt_keys[2], head_w, qk_scale).astype(jnp.bfloat16),
        'b_q': draw_normal(wt_keys[3], head_b, 0.5).astype(jnp.bfloat16),
        'w_k': draw_normal(wt_keys[4], head_w, qk_scale).astype(jnp.bfloat16),
        'w_v': draw_normal(wt_keys[5], head_w, in_scale).astype(jnp.bfloat16),
        'b_v': draw_normal(wt_keys[6], head_b, 0.5).astype(jnp.bfloat16),
        'w_o': draw_normal(wt_keys[7], (NUM_HEADS, HEAD_DIM, WIDTH), 2.5 * in_scale).astype(jnp.bfloat16),
        'b_o': draw_normal(wt_keys[8], (WIDTH,), 0.5).astype(jnp.bfloat16),
        'ln2_gain': 1.0 + draw_normal(wt_keys[9], (WIDTH,), 0.25),
        'ln2_bias': draw_normal(wt_keys[10], (WIDTH,), 0.3),
        'w_1': draw_normal(wt_keys[11], (WIDTH, MLP_DIM), in_scale).astype(jnp.bfloat16),
        'b_1': draw_normal(wt_keys[12], (MLP_DIM,), 0.5).astype(jnp.bfloat16),
        'w_2': draw_normal(wt_keys[13], (MLP_DIM, WIDTH), 1.5 * MLP_DIM ** -0.5).astype(jnp.bfloat16),
        'b_2': draw_normal(wt_keys[14], (WIDTH,), 0.5).astype(jnp.bfloat16),
    }


def layer_norm(rows, ln_gain, ln_bias):
    row_mean = jnp.mean(rows, axis=-1, keepdims=True)
    centered = rows - row_mean
    variance = jnp.mean(centered * centered, axis=-1, keepdims=True)
    return centered * lax.rsqrt(variance + LN_EPS) * ln_gain + ln_bias


def attend_image(qkv_image):
    queries, keys, values = qkv_image
    scores = jnp.einsum('qhd,khd->hqk', queries.astype(jnp.float32), keys.astype(jnp.float32)) * ATT_SCALE
    probs = jax.nn.softmax(scores, axis=-1).astype(jnp.bfloat16)
    mixed = jnp.einsum('hqk,khd->qhd', probs.astype(jnp.float32), values.astype(jnp.float32))
    return mixed.astype(jnp.bfloat16)


def forward(x, ln1_gain, ln1_bias, w_q, b_q, w_k, w_v, b_v, w_o, b_o, ln2_gain, ln2_bias, w_1, b_1, w_2, b_2):
    x_f32 = x.reshape(TOKENS, WIDTH).astype(jnp.float32)
    h_one = layer_norm(x_f32, ln1_gain, ln1_bias).astype(jnp.bfloat16)
    w_qkv = jnp.concatenate([w_q.reshape(WIDTH, WIDTH), w_k.reshape(WIDTH, WIDTH), w_v.reshape(WIDTH, WIDTH)], axis=1)
    b_qkv = jnp.concatenate([b_q.reshape(WIDTH).astype(jnp.float32), jnp.zeros((WIDTH,), jnp.float32), b_v.reshape(WIDTH).astype(jnp.float32)])
    qkv = (jnp.dot(h_one, w_qkv, preferred_element_type=jnp.float32) + b_qkv).astype(jnp.bfloat16)
    head_shape = (IMAGES, PATCHES, NUM_HEADS, HEAD_DIM)
    queries = qkv[:, :WIDTH].reshape(head_shape)
    keys = qkv[:, WIDTH:2 * WIDTH].reshape(head_shape)
    values = qkv[:, 2 * WIDTH:].reshape(head_shape)
    mixed = lax.map(attend_image, (queries, keys, values)).reshape(TOKENS, WIDTH)
    attn_out = jnp.dot(mixed, w_o.reshape(WIDTH, WIDTH), preferred_element_type=jnp.float32)
    x_mid = (x_f32 + attn_out + b_o).astype(jnp.bfloat16)
    mid_f32 = x_mid.astype(jnp.float32)
    h_two = layer_norm(mid_f32, ln2_gain, ln2_bias).astype(jnp.bfloat16)
    pre_act = (jnp.dot(h_two, w_1, preferred_element_type=jnp.float32) + b_1).astype(jnp.bfloat16)
    hidden = jax.nn.gelu(pre_act.astype(jnp.float32), approximate=True).astype(jnp.bfloat16)
    mlp_out = jnp.dot(hidden, w_2, preferred_element_type=jnp.float32)
    y_out = (mid_f32 + mlp_out + b_2).astype(jnp.bfloat16)
    return y_out.reshape(IMAGES, PATCHES, WIDTH)


def reference(x, d_out, ln1_gain, ln1_bias, w_q, b_q, w_k, w_v, b_v, w_o, b_o, ln2_gain, ln2_bias, w_1, b_1, w_2, b_2):
    y_out, pullback = jax.vjp(forward, x, ln1_gain, ln1_bias, w_q, b_q, w_k, w_v, b_v, w_o, b_o, ln2_gain, ln2_bias, w_1, b_1, w_2, b_2)
    (grad_x, grad_ln1_gain, grad_ln1_bias, grad_w_q, grad_b_q, grad_w_k, grad_w_v, grad_b_v, grad_w_o, grad_b_o,
     grad_ln2_gain, grad_ln2_bias, grad_w_1, grad_b_1, grad_w_2, grad_b_2) = pullback(d_out)
    return (y_out, grad_x, grad_ln1_gain, grad_ln1_bias, grad_w_q, grad_b_q, grad_w_k, grad_w_v, grad_b_v, grad_w_o, grad_b_o,
            grad_ln2_gain, grad_ln2_bias, grad_w_1, grad_b_1, grad_w_2, grad_b_2)
```

```python
import math
import numpy as np
import jax
import jax.numpy as jnp
from jax import lax
from jax.sharding import Mesh, PartitionSpec as P

LN_EPS = 1e-6
BF16 = jnp.bfloat16
F32 = jnp.float32

CHIPS = 4
HEADS = 2
HEAD_DIM = 72
QROWS = HEADS * HEAD_DIM
WIDTH = 1152
MLP = 538
MLP_PAD = 544
HALF = MLP_PAD // 2
ALL_AXES = ('dp', 'chip', 'core')


def layer_norm(rows, ln_gain, ln_bias):
    row_mean = jnp.mean(rows, axis=-1, keepdims=True)
    centered = rows - row_mean
    variance = jnp.mean(centered * centered, axis=-1, keepdims=True)
    return centered * lax.rsqrt(variance + LN_EPS) * ln_gain + ln_bias


def gelu_tanh(pre_act):
    return jax.nn.gelu(pre_act, approximate=True)


def attention_core(queries, keys, values):
    att_scale = 1.0 / math.sqrt(queries.shape[-1])
    scores = jnp.einsum('bqhd,bkhd->bhqk', queries, keys, preferred_element_type=F32) * att_scale
    probs = jax.nn.softmax(scores, axis=-1).astype(BF16)
    mixed = jnp.einsum('bhqk,bkhd->bqhd', probs, values, preferred_element_type=F32)
    return mixed.astype(BF16)


def tie(val, *deps):
    return lax.optimization_barrier((val,) + deps)[0]


def dot_t(a, b):
    return lax.dot_general(a, b, (((1,), (1,)), ((), ())), preferred_element_type=F32)


def dot_n(a, b):
    return lax.dot_general(a, b, (((1,), (0,)), ((), ())), preferred_element_type=F32)


def dot_w(a, b):
    return lax.dot_general(a, b, (((0,), (0,)), ((), ())), preferred_element_type=F32)


def solution(mesh):
    mesh3 = Mesh(mesh.devices.reshape(2, CHIPS, 2), ALL_AXES)
    tp = ('chip', 'core')
    act_spec = P('dp', tp, None)
    replicated = P()
    head_w = P(None, tp, None)
    head_b = P(tp, None)
    grad_head_w = P('dp', tp, None)
    dp_tp = ('dp', 'chip', 'core')
    grad_head_b = P(dp_tp, None)
    grad_vec = P('dp')
    in_specs = (act_spec, act_spec, replicated, replicated, head_w, head_b, head_w, head_w, head_b,
                P(tp, None, None), replicated, replicated, replicated, P(None, tp), P(tp), P(tp, None), replicated)
    out_specs = (act_spec, act_spec, grad_vec, grad_vec, grad_head_w, grad_head_b, grad_head_w, grad_head_w, grad_head_b,
                 P(dp_tp, None, None), grad_vec, grad_vec, grad_vec, P('dp', tp), P(dp_tp),
                 P(dp_tp, None), grad_vec)

    def tp_perm(fn):
        return [(i, fn(i)) for i in range(8)]

    def permute(val, fn):
        return lax.ppermute(val, tp, tp_perm(fn))

    def core_swap(val):
        return permute(val, lambda i: i ^ 1)

    def pick(val, idx, axis=0):
        return lax.dynamic_index_in_dim(val, idx, axis, keepdims=False)

    def layer_step(x, d_out, ln1_gain, ln1_bias, w_q, b_q, w_k, w_v, b_v, w_o, b_o, ln2_gain, ln2_bias, w_1, b_1, w_2, b_2):
        dp = lax.axis_index('dp')
        chip = lax.axis_index('chip')
        core = lax.axis_index('core')
        cx, cy = chip % 2, chip // 2
        rank = chip * 2 + core
        core0 = core == 0
        images = x.shape[0] // 8
        toks = x.shape[1]
        rows = images * toks * 8

        def to_images(val):
            blocks = val.reshape(8, images, toks, WIDTH)
            out = jnp.zeros((images, 8, toks, WIDTH), val.dtype)
            for k in range(8):
                piece = pick(blocks, rank ^ k)
                if k:
                    piece = permute(piece, lambda i: i ^ k)
                out = lax.dynamic_update_slice(out, piece[:, None], (0, rank ^ k, 0, 0))
            return out.reshape(rows, WIDTH)

        def to_tokens(val):
            blocks = val.reshape(images, 8, toks, WIDTH)
            out = jnp.zeros((8, images, toks, WIDTH), val.dtype)
            for k in range(8):
                piece = pick(blocks, rank ^ k, 1)
                if k:
                    piece = permute(piece, lambda i: i ^ k)
                out = lax.dynamic_update_slice(out, piece[None], (rank ^ k, 0, 0, 0))
            return out.reshape(8 * images, toks, WIDTH)

        first = lambda i: (i ^ 2) if i % 2 == 0 else (i ^ 4)
        second = lambda i: (i ^ 4) if i % 2 == 0 else (i ^ 2)
        me = jnp.where(core0, cy, cx)
        away = lambda k: jnp.where(core0, k * 2 + (1 - cx), (1 - cy) * 2 + k)
        near = lambda k: jnp.where(core0, k * 2 + cx, cy * 2 + k)

        def stage1(other):
            return core_swap(other)

        def stage2(own, got, axis):
            blk = lambda i: pick(own, i, axis) + pick(got, i, axis)
            send = (blk(away(1 - me)), blk(away(me)))
            return send, tuple(permute(v, first) for v in send)

        def stage3(own, got, axis, far):
            send = pick(own, near(1 - me), axis) + pick(got, near(1 - me), axis) + far
            return send, permute(send, second)

        def finish(own, got, axis, close, part):
            return pick(own, near(me), axis) + pick(got, near(me), axis) + close + part

        def gather(half0, half1, *after):
            mine = jnp.where(dp == 0, half0, half1)
            if after:
                mine = tie(mine, *after)
            own = lax.all_gather(mine, ('dp', 'chip'), axis=0, tiled=False)
            own = own.reshape(2, CHIPS, *mine.shape)
            return own, core_swap(own)

        def rows_of(w):
            return jnp.transpose(w, (1, 2, 0)).reshape(QROWS, WIDTH)

        b1_pad = jnp.pad(b_1, (0, MLP_PAD - MLP))

        def bias_rows(head_bias, mlp_bias):
            row = jnp.concatenate([head_bias.reshape(QROWS), mlp_bias])
            return jnp.pad(row[None], ((0, 15), (0, WIDTH - row.shape[0])))

        att0 = jnp.concatenate([rows_of(w_q), rows_of(w_k), bias_rows(b_q, b1_pad[:HALF])])
        att1 = jnp.concatenate([rows_of(w_v), w_o.reshape(QROWS, WIDTH), bias_rows(b_v, b1_pad[HALF:])])
        att = gather(att0, att1)
        w1_rows = jnp.pad(w_1.T, ((0, MLP_PAD - MLP), (0, 0)))
        w2_rows = jnp.pad(w_2, ((0, MLP_PAD - MLP), (0, 0)))
        w1_all = [w.reshape(2 * CHIPS * HALF, WIDTH) for w in gather(w1_rows[:HALF], w1_rows[HALF:], att[0])]
        w2_all = [w.reshape(2 * CHIPS * HALF, WIDTH) for w in gather(w2_rows[:HALF], w2_rows[HALF:], w1_all[0])]

        flat = CHIPS * QROWS
        wqkv = [jnp.concatenate([a[0, :, :QROWS].reshape(flat, WIDTH), a[0, :, QROWS:2 * QROWS].reshape(flat, WIDTH),
                                 a[1, :, :QROWS].reshape(flat, WIDTH)]) for a in att]
        wo = [a[1, :, QROWS:2 * QROWS].reshape(flat, WIDTH) for a in att]
        bqkv = [jnp.concatenate([a[0, :, 2 * QROWS, :QROWS].reshape(flat), jnp.zeros((flat,), BF16),
                                 a[1, :, 2 * QROWS, :QROWS].reshape(flat)]).astype(F32) for a in att]
        b1_all = [a[:, :, 2 * QROWS, QROWS:QROWS + HALF].reshape(2 * CHIPS * HALF).astype(F32) for a in att]

        x_rows = to_images(x)
        g_out = to_images(tie(d_out, att[0]))

        x_f32 = x_rows.astype(F32)
        h_one_f, ln1_pull = jax.vjp(layer_norm, x_f32, ln1_gain, ln1_bias)
        h_one = h_one_f.astype(BF16)
        qkv = [(dot_t(h_one, w) + b).astype(BF16) for w, b in zip(wqkv, bqkv)]
        packed = jnp.stack([t.reshape(images, 8 * toks, 3, CHIPS * HEADS, HEAD_DIM) for t in qkv], axis=2)
        heads = lambda part: packed[:, :, :, part].reshape(images, 8 * toks, 16, HEAD_DIM)
        mixed, attn_pull = jax.vjp(attention_core, heads(0), heads(1), heads(2))
        mixed = mixed.reshape(rows, 16 * HEAD_DIM)
        wo_all = jnp.concatenate(wo)
        attn_out = dot_n(mixed, wo_all)
        x_mid = (x_f32 + attn_out + b_o).astype(BF16)
        mid_f32 = x_mid.astype(F32)
        h_two_f, ln2_pull = jax.vjp(layer_norm, mid_f32, ln2_gain, ln2_bias)
        h_two = h_two_f.astype(BF16)
        blocks = (2, CHIPS, HALF, WIDTH)
        hidden, gelu_pulls = [], []
        for w1, b1 in zip(w1_all, b1_all):
            pre_act = (dot_t(h_two, w1) + b1).astype(BF16)
            hid_f, gelu_pull = jax.vjp(gelu_tanh, pre_act.astype(F32))
            hidden.append(hid_f.astype(BF16))
            gelu_pulls.append(gelu_pull)
        w2_oth = dot_w(hidden[1], g_out).reshape(blocks)
        w2_got = stage1(w2_oth)
        w2_own = dot_w(tie(hidden[0], w2_oth), g_out).reshape(blocks)
        w2_send, w2_in = stage2(w2_own, w2_got, 1)
        g_mlp = tie(g_out, *w2_send)
        d_pre = [None, None]
        for c in (1, 0):
            d_hidden = dot_t(g_mlp, w2_all[c]).astype(BF16)
            (d_pre_f,) = gelu_pulls[c](d_hidden.astype(F32))
            d_pre[c] = d_pre_f.astype(BF16)
        w1_oth = dot_w(d_pre[1], h_two).reshape(blocks)
        w1_got = stage1(w1_oth)
        w1_own = dot_w(tie(d_pre[0], w1_oth), h_two).reshape(blocks)
        d_pre_t = [tie(d, w1_own) for d in d_pre]
        d_h_two = (dot_n(d_pre_t[0], w1_all[0]) + dot_n(d_pre_t[1], w1_all[1])).astype(BF16)
        d_mid_ln, g_ln2_gain, g_ln2_bias = ln2_pull(d_h_two.astype(F32))
        d_mid = (g_out.astype(F32) + d_mid_ln).astype(BF16)
        d_mixed = dot_t(d_mid, wo_all).astype(BF16)
        wo_oth = dot_w(mixed[:, flat:], d_mid).reshape(CHIPS, QROWS, WIDTH)
        wo_got = stage1(wo_oth)
        wo_own = dot_w(mixed[:, :flat], d_mid).reshape(CHIPS, QROWS, WIDTH)
        w1_send, w1_in = stage2(w1_own, w1_got, 1)
        w2_last, w2_part = stage3(w2_own, w2_got, 1, w2_in[0])
        wo_send, wo_in = stage2(wo_own, wo_got, 0)
        d_heads = attn_pull(tie(d_mixed, *w1_send, w2_last, *wo_send).reshape(images, 8 * toks, 16, HEAD_DIM))
        d_packed = jnp.stack([t.reshape(rows, 2, flat) for t in d_heads], axis=2)
        d_qkv = [d_packed[:, c].reshape(rows, 3 * flat) for c in range(2)]
        w1_last, w1_part = stage3(w1_own, w1_got, 1, w1_in[0])
        wo_last, wo_part = stage3(wo_own, wo_got, 0, wo_in[0])
        d_qkv = list(lax.optimization_barrier((*d_qkv, w1_last, wo_last))[:2])
        qkv_blocks = (3, CHIPS, QROWS, WIDTH)
        qkv_oth = dot_w(d_qkv[1], h_one).reshape(qkv_blocks)
        qkv_got = stage1(qkv_oth)
        qkv_own = dot_w(tie(d_qkv[0], qkv_oth), h_one).reshape(qkv_blocks)
        d_qkv_t = [tie(d, qkv_own) for d in d_qkv]
        d_h_one = (dot_n(d_qkv_t[0], wqkv[0]) + dot_n(d_qkv_t[1], wqkv[1])).astype(BF16)
        qkv_send, qkv_in = stage2(qkv_own, qkv_got, 1)
        d_h_one = tie(d_h_one, *qkv_send)
        d_in_ln, g_ln1_gain, g_ln1_bias = ln1_pull(d_h_one.astype(F32))
        g_x = (d_mid.astype(F32) + d_in_ln).astype(BF16)
        grad_x = to_tokens(g_x)
        mlp_out = dot_n(tie(hidden[0], g_x), w2_all[0]) + dot_n(hidden[1], w2_all[1])
        y_rows = (mid_f32 + mlp_out + b_2).astype(BF16)
        y_out = to_tokens(y_rows)
        qkv_last, qkv_part = stage3(qkv_own, qkv_got, 1, qkv_in[0])

        grad_w2 = finish(w2_own, w2_got, 1, w2_in[1], w2_part)
        grad_w2 = grad_w2.reshape(MLP_PAD, WIDTH)[:MLP].astype(BF16)
        grad_w1 = finish(w1_own, w1_got, 1, w1_in[1], w1_part)
        grad_w1 = grad_w1.reshape(MLP_PAD, WIDTH)[:MLP].T.astype(BF16)
        grad_wo = finish(wo_own, wo_got, 0, wo_in[1], wo_part)
        grad_wo = grad_wo.reshape(HEADS, HEAD_DIM, WIDTH).astype(BF16)
        grad_qkv = finish(qkv_own, qkv_got, 1, qkv_in[1], qkv_part).astype(BF16)
        unrow = lambda w: jnp.transpose(w.reshape(HEADS, HEAD_DIM, WIDTH), (2, 0, 1))

        col_sum = lambda v: jnp.sum(v, axis=0, dtype=F32)
        vecs = jnp.stack([g_ln1_gain, g_ln1_bias, col_sum(d_mid), g_ln2_gain, g_ln2_bias, col_sum(g_out)])

        def extra_rows(c):
            sums = col_sum(d_qkv[c]).reshape(3, CHIPS, QROWS)
            b1_sum = jnp.transpose(col_sum(d_pre[c]).reshape(2, CHIPS, HALF), (1, 0, 2)).reshape(CHIPS, MLP_PAD)
            row = jnp.concatenate([sums[0], sums[2], b1_sum, jnp.zeros((CHIPS, WIDTH - 2 * QROWS - MLP_PAD), F32)], axis=1)
            return jnp.concatenate([jnp.broadcast_to(vecs, (CHIPS, 6, WIDTH)), row[:, None],
                                    jnp.zeros((CHIPS, 1, WIDTH), F32)], axis=1)

        ex_own, ex_got = extra_rows(0), stage1(extra_rows(1))
        _, ex_in = stage2(ex_own, ex_got, 0)
        _, ex_part = stage3(ex_own, ex_got, 0, ex_in[0])
        extra = finish(ex_own, ex_got, 0, ex_in[1], ex_part)
        b_row = extra[6].astype(BF16)
        return (y_out, grad_x, extra[0], extra[1], unrow(grad_qkv[0]), b_row[:QROWS].reshape(HEADS, HEAD_DIM),
                unrow(grad_qkv[1]), unrow(grad_qkv[2]), b_row[QROWS:2 * QROWS].reshape(HEADS, HEAD_DIM), grad_wo,
                extra[2].astype(BF16), extra[3], extra[4], grad_w1, b_row[2 * QROWS:2 * QROWS + MLP], grad_w2,
                extra[5].astype(BF16))

    return jax.shard_map(layer_step, mesh=mesh3, in_specs=in_specs, out_specs=out_specs, check_vma=False)
```

```python
import math
import jax
import jax.numpy as jnp
from jax import lax
from jax.experimental import pallas as pl
from jax.experimental.pallas import tpu as pltpu
from jax.sharding import Mesh, PartitionSpec as P

LN_EPS = 1e-6
BF16 = jnp.bfloat16
F32 = jnp.float32

CHIPS = 4
HEADS = 2
HEAD_DIM = 72
QROWS = HEADS * HEAD_DIM
WIDTH = 1152
MLP = 538
MLP_PAD = 544
HALF = MLP_PAD // 2
ALL_AXES = ('dp', 'chip', 'core')
N_HEADS = 16
WIN_LANES = 256
ATT_SCALE = 1.0 / math.sqrt(HEAD_DIM)


def layer_norm(rows, ln_gain, ln_bias):
    row_mean = jnp.mean(rows, axis=-1, keepdims=True)
    centered = rows - row_mean
    variance = jnp.mean(centered * centered, axis=-1, keepdims=True)
    return centered * lax.rsqrt(variance + LN_EPS) * ln_gain + ln_bias


def gelu_tanh(pre_act):
    return jax.nn.gelu(pre_act, approximate=True)


def dot_nt(a, b):
    return lax.dot_general(a, b, (((1,), (1,)), ((), ())), preferred_element_type=F32)
def dot_nn(a, b):
    return lax.dot_general(a, b, (((1,), (0,)), ((), ())), preferred_element_type=F32)
def dot_tn(a, b):
    return lax.dot_general(a, b, (((0,), (0,)), ((), ())), preferred_element_type=F32)

def head_window(head):
    low = head * HEAD_DIM
    base = jnp.minimum(low // 128, WIDTH // 128 - 2) * 128
    base = pl.multiple_of(base, 128)
    lane = lax.broadcasted_iota(jnp.int32, (1, WIN_LANES), 1)
    mask = (lane >= low - base) & (lane < low - base + HEAD_DIM)
    return pl.ds(base, WIN_LANES), base, mask

def probs_t(keys, queries):
    scores = dot_nt(keys, queries) * ATT_SCALE
    scores = jnp.exp(scores - jnp.max(scores, axis=0, keepdims=True))
    return scores * (1.0 / jnp.sum(scores, axis=0, keepdims=True))

def attn_fwd(q_ref, k_ref, v_ref, out_ref, acc):
    acc[...] = jnp.zeros_like(acc)

    def body(head, _):
        win, _, mask = head_window(head)
        zero = jnp.zeros((), BF16)
        keys = jnp.where(mask, k_ref[:, win], zero)
        vals = jnp.where(mask, v_ref[:, win], zero)
        probs = probs_t(keys, q_ref[:, win]).astype(BF16)
        acc[:, win] += dot_tn(probs, vals)
        return 0

    lax.fori_loop(0, N_HEADS, body, 0, unroll=2)
    out_ref[...] = acc[...].astype(BF16)

def attn_bwd(q_ref, k_ref, v_ref, do_ref, out_ref, acc):
    acc[...] = jnp.zeros_like(acc)

    def body(head, _):
        win, base, mask = head_window(head)
        zero = jnp.zeros((), BF16)
        queries = jnp.where(mask, q_ref[:, win], zero)
        keys = jnp.where(mask, k_ref[:, win], zero)
        d_out = jnp.where(mask, do_ref[:, win], zero)
        probs = probs_t(keys, queries)
        d_probs = dot_nt(v_ref[:, win], d_out).astype(BF16).astype(F32)
        prod = d_probs * probs
        d_scores = (prod - probs * jnp.sum(prod, axis=0, keepdims=True)) * ATT_SCALE
        d_scores = d_scores.astype(BF16)
        acc[:, win] += dot_tn(d_scores, keys)
        acc[:, pl.ds(pl.multiple_of(base + WIDTH, 128), WIN_LANES)] += dot_nn(d_scores, queries)
        acc[:, pl.ds(pl.multiple_of(base + 2 * WIDTH, 128), WIN_LANES)] += dot_nn(probs.astype(BF16), d_out)
        return 0

    lax.fori_loop(0, N_HEADS, body, 0, unroll=2)
    out_ref[...] = acc[...].astype(BF16)

def part_spec(toks, part):
    return pl.BlockSpec((toks, WIDTH), lambda i: (i, part))

def attention_forward(qkv, toks):
    rows = qkv.shape[0]
    flops = 2 * 2 * rows * toks * 256 * N_HEADS
    return pl.pallas_call(attn_fwd, grid=(rows // toks,), out_shape=jax.ShapeDtypeStruct((rows, WIDTH), BF16),
        in_specs=[part_spec(toks, p) for p in range(3)], out_specs=part_spec(toks, 0),
        scratch_shapes=[pltpu.VMEM((toks, WIDTH), F32)], name='attn_fwd',
        cost_estimate=pl.CostEstimate(flops=4*flops, bytes_accessed=rows * WIDTH * 8, transcendentals=rows * toks * N_HEADS),
    )(qkv, qkv, qkv)

def attention_backward(qkv, d_mixed, toks):
    rows = qkv.shape[0]
    flops = 5 * 2 * rows * toks * 256 * N_HEADS
    return pl.pallas_call(attn_bwd, grid=(rows // toks,), out_shape=jax.ShapeDtypeStruct((rows, 3 * WIDTH), BF16),
        in_specs=[part_spec(toks, p) for p in range(3)] + [part_spec(toks, 0)],
        out_specs=pl.BlockSpec((toks, 3 * WIDTH), lambda i: (i, 0)),
        scratch_shapes=[pltpu.VMEM((toks, 3 * WIDTH), F32)], name='attn_bwd',
        cost_estimate=pl.CostEstimate(flops=4*flops, bytes_accessed=rows * WIDTH * 14, transcendentals=rows * toks * N_HEADS),
    )(qkv, qkv, qkv, d_mixed)


def tie(val, *deps):
    return lax.optimization_barrier((val,) + deps)[0]


def solution(mesh):
    mesh3 = Mesh(mesh.devices.reshape(2, CHIPS, 2), ALL_AXES)
    tp = ('chip', 'core')
    act_spec = P('dp', tp, None)
    replicated = P()
    head_w = P(None, tp, None)
    head_b = P(tp, None)
    grad_head_w = P('dp', tp, None)
    dp_tp = ('dp', 'chip', 'core')
    grad_head_b = P(dp_tp, None)
    grad_vec = P('dp')
    in_specs = (act_spec, act_spec, replicated, replicated, head_w, head_b, head_w, head_w, head_b,
                P(tp, None, None), replicated, replicated, replicated, P(None, tp), P(tp), P(tp, None), replicated)
    out_specs = (act_spec, act_spec, grad_vec, grad_vec, grad_head_w, grad_head_b, grad_head_w, grad_head_w, grad_head_b,
                 P(dp_tp, None, None), grad_vec, grad_vec, grad_vec, P('dp', tp), P(dp_tp),
                 P(dp_tp, None), grad_vec)

    def tp_perm(fn):
        return [(i, fn(i)) for i in range(8)]

    def permute(val, fn):
        return lax.ppermute(val, tp, tp_perm(fn))

    def core_swap(val):
        return permute(val, lambda i: i ^ 1)

    def pick(val, idx, axis=0):
        return lax.dynamic_index_in_dim(val, idx, axis, keepdims=False)

    def layer_step(x, d_out, ln1_gain, ln1_bias, w_q, b_q, w_k, w_v, b_v, w_o, b_o, ln2_gain, ln2_bias, w_1, b_1, w_2, b_2):
        dp = lax.axis_index('dp')
        chip = lax.axis_index('chip')
        core = lax.axis_index('core')
        cx, cy = chip % 2, chip // 2
        rank = chip * 2 + core
        core0 = core == 0
        images = x.shape[0] // 8
        toks = x.shape[1]
        rows = images * toks * 8

        def to_images(val):
            blocks = val.reshape(8, images, toks, WIDTH)
            pieces = []
            for k in range(8):
                piece = pick(blocks, rank ^ k)
                if k:
                    piece = permute(piece, lambda i: i ^ k)
                pieces.append(piece[:, None])
            return jnp.concatenate(pieces, axis=1).reshape(rows, WIDTH)

        def to_tokens(val):
            blocks = val.reshape(images, 8, toks, WIDTH)
            pieces = []
            for k in range(8):
                piece = blocks[:, k]
                if k:
                    piece = permute(piece, lambda i: i ^ k)
                pieces.append(piece)
            for bit in (1, 2, 4):
                odd = (rank & bit) != 0
                pieces = [jnp.where(odd, pieces[k ^ bit], pieces[k]) for k in range(8)]
            return jnp.concatenate(pieces, axis=0)

        first = lambda i: (i ^ 2) if i % 2 == 0 else (i ^ 4)
        second = lambda i: (i ^ 4) if i % 2 == 0 else (i ^ 2)
        me = jnp.where(core0, cy, cx)
        away = lambda k: jnp.where(core0, k * 2 + (1 - cx), (1 - cy) * 2 + k)
        near = lambda k: jnp.where(core0, k * 2 + cx, cy * 2 + k)

        def stage2(own, got, axis):
            blk = lambda i: pick(own, i, axis) + pick(got, i, axis)
            send = (blk(away(1 - me)), blk(away(me)))
            far = permute(send[0], first)
            close = permute(send[1], first)
            return send, (far, close)

        def stage3(own, got, axis, far):
            send = pick(own, near(1 - me), axis) + pick(got, near(1 - me), axis) + far
            return send, permute(send, second)

        def finish(own, got, axis, close, part):
            return pick(own, near(me), axis) + pick(got, near(me), axis) + close + part

        def gather(half0, half1):
            mine = jnp.where(dp == 0, half0, half1)
            own = lax.all_gather(mine, ('dp', 'chip'), axis=0, tiled=False)
            own = own.reshape(2, CHIPS, *mine.shape)
            return own, core_swap(own)

        def rows_of(w):
            return jnp.transpose(w, (1, 2, 0)).reshape(QROWS, WIDTH)

        b1_pad = jnp.pad(b_1, (0, MLP_PAD - MLP))

        def bias_rows(head_bias, mlp_bias):
            row = jnp.concatenate([head_bias.reshape(QROWS), mlp_bias])
            return jnp.pad(row[None], ((0, 15), (0, WIDTH - row.shape[0])))

        att0 = jnp.concatenate([rows_of(w_q), rows_of(w_k), bias_rows(b_q, b1_pad[:HALF])])
        att1 = jnp.concatenate([rows_of(w_v), w_o.reshape(QROWS, WIDTH), bias_rows(b_v, b1_pad[HALF:])])
        att = gather(att0, att1)
        w1_rows = jnp.pad(w_1.T, ((0, MLP_PAD - MLP), (0, 0)))
        w2_rows = jnp.pad(w_2, ((0, MLP_PAD - MLP), (0, 0)))
        w1_all = [w.reshape(2 * CHIPS * HALF, WIDTH) for w in gather(w1_rows[:HALF], w1_rows[HALF:])]
        w2_all = [w.reshape(2 * CHIPS * HALF, WIDTH) for w in gather(w2_rows[:HALF], w2_rows[HALF:])]

        flat = CHIPS * QROWS
        part = lambda half, first: [a[half, :, first:first + QROWS].reshape(flat, WIDTH) for a in att]
        bias = lambda half: [a[half, :, 2 * QROWS, :QROWS].reshape(flat) for a in att]
        wqkv = jnp.concatenate(part(0, 0) + part(0, QROWS) + part(1, 0))
        wo_all = jnp.concatenate(part(1, QROWS))
        bqkv = jnp.concatenate(bias(0) + [jnp.zeros((2 * flat,), BF16)] + bias(1)).astype(F32)
        b1_all = [a[:, :, 2 * QROWS, QROWS:QROWS + HALF].reshape(2 * CHIPS * HALF).astype(F32) for a in att]

        x_rows = to_images(x)
        g_out = to_images(tie(d_out, att[0]))

        x_f32 = x_rows.astype(F32)
        h_one_f, ln1_pull = jax.vjp(layer_norm, x_f32, ln1_gain, ln1_bias)
        h_one = h_one_f.astype(BF16)
        qkv = (dot_nt(h_one, wqkv) + bqkv).astype(BF16)
        mixed = attention_forward(qkv, 8 * toks)
        attn_out = dot_nn(mixed, wo_all)
        x_mid = (x_f32 + attn_out + b_o).astype(BF16)
        mid_f32 = x_mid.astype(F32)
        h_two_f, ln2_pull = jax.vjp(layer_norm, mid_f32, ln2_gain, ln2_bias)
        h_two = h_two_f.astype(BF16)
        blocks = (2, CHIPS, HALF, WIDTH)
        hidden, gelu_pulls = [], []
        for w1, b1 in zip(w1_all, b1_all):
            pre_act = (dot_nt(h_two, w1) + b1).astype(BF16)
            hid_f, gelu_pull = jax.vjp(gelu_tanh, pre_act.astype(F32))
            hidden.append(hid_f.astype(BF16))
            gelu_pulls.append(gelu_pull)
        w2_oth = dot_tn(hidden[1], g_out).reshape(blocks)
        w2_got = core_swap(w2_oth)
        w2_own = dot_tn(tie(hidden[0], w2_oth), g_out).reshape(blocks)
        w2_send, w2_in = stage2(w2_own, w2_got, 1)
        g_mlp = tie(g_out, *w2_send)
        d_pre = [None, None]
        for c in (1, 0):
            d_hidden = dot_nt(g_mlp, w2_all[c]).astype(BF16)
            (d_pre_f,) = gelu_pulls[c](d_hidden.astype(F32))
            d_pre[c] = d_pre_f.astype(BF16)
        w1_oth = dot_tn(d_pre[1], h_two).reshape(blocks)
        w1_got = core_swap(w1_oth)
        w1_own = dot_tn(tie(d_pre[0], w1_oth), h_two).reshape(blocks)
        w1_send, w1_in = stage2(w1_own, w1_got, 1)
        d_pre_t = [tie(d, *w1_send) for d in d_pre]
        d_h_two = (dot_nn(d_pre_t[0], w1_all[0]) + dot_nn(d_pre_t[1], w1_all[1])).astype(BF16)
        d_mid_ln, g_ln2_gain, g_ln2_bias = ln2_pull(d_h_two.astype(F32))
        d_mid = (g_out.astype(F32) + d_mid_ln).astype(BF16)
        d_mixed = dot_nt(d_mid, wo_all).astype(BF16)
        wo_oth = dot_tn(mixed[:, flat:], d_mid).reshape(CHIPS, QROWS, WIDTH)
        wo_got = core_swap(wo_oth)
        wo_own = dot_tn(mixed[:, :flat], d_mid).reshape(CHIPS, QROWS, WIDTH)
        w2_last, w2_part = stage3(w2_own, w2_got, 1, w2_in[0])
        wo_send, wo_in = stage2(wo_own, wo_got, 0)
        d_qkv = attention_backward(qkv, tie(d_mixed, w2_last, *wo_send), 8 * toks)
        w1_last, w1_part = stage3(w1_own, w1_got, 1, w1_in[0])
        wo_last, wo_part = stage3(wo_own, wo_got, 0, wo_in[0])
        d_qkv = tie(d_qkv, w1_last, wo_last)
        dw_qkv = dot_tn(d_qkv, h_one).reshape(3, 2, CHIPS, QROWS, WIDTH)
        qkv_own, qkv_oth = dw_qkv[:, 0], dw_qkv[:, 1]
        qkv_got = core_swap(qkv_oth)
        d_h_one = dot_nn(tie(d_qkv, qkv_oth), wqkv).astype(BF16)
        qkv_send, qkv_in = stage2(qkv_own, qkv_got, 1)
        d_h_one = tie(d_h_one, *qkv_send)
        d_in_ln, g_ln1_gain, g_ln1_bias = ln1_pull(d_h_one.astype(F32))
        g_x = (d_mid.astype(F32) + d_in_ln).astype(BF16)
        grad_x = to_tokens(g_x)
        mlp_out = dot_nn(tie(hidden[0], d_h_one), w2_all[0])
        mlp_out = mlp_out + dot_nn(hidden[1], w2_all[1])
        y_rows = (mid_f32 + mlp_out + b_2).astype(BF16)
        y_out = to_tokens(y_rows)
        _, qkv_part = stage3(qkv_own, qkv_got, 1, qkv_in[0])

        grad_w2 = finish(w2_own, w2_got, 1, w2_in[1], w2_part)
        grad_w2 = grad_w2.reshape(MLP_PAD, WIDTH)[:MLP].astype(BF16)
        grad_w1 = finish(w1_own, w1_got, 1, w1_in[1], w1_part)
        grad_w1 = grad_w1.reshape(MLP_PAD, WIDTH)[:MLP].T.astype(BF16)
        grad_wo = finish(wo_own, wo_got, 0, wo_in[1], wo_part)
        grad_wo = grad_wo.reshape(HEADS, HEAD_DIM, WIDTH).astype(BF16)
        grad_qkv = finish(qkv_own, qkv_got, 1, qkv_in[1], qkv_part).astype(BF16)
        unrow = lambda w: jnp.transpose(w.reshape(HEADS, HEAD_DIM, WIDTH), (2, 0, 1))

        col_sum = lambda v: jnp.sum(v, axis=0, dtype=F32)
        vecs = jnp.stack([g_ln1_gain, g_ln1_bias, col_sum(d_mid), g_ln2_gain, g_ln2_bias, col_sum(g_out)])

        qkv_sums = col_sum(d_qkv).reshape(3, 2, CHIPS, QROWS)

        def extra_rows(c):
            sums = qkv_sums[:, c]
            b1_sum = jnp.transpose(col_sum(d_pre[c]).reshape(2, CHIPS, HALF), (1, 0, 2)).reshape(CHIPS, MLP_PAD)
            row = jnp.concatenate([sums[0], sums[2], b1_sum, jnp.zeros((CHIPS, WIDTH - 2 * QROWS - MLP_PAD), F32)], axis=1)
            return jnp.concatenate([jnp.broadcast_to(vecs, (CHIPS, 6, WIDTH)), row[:, None],
                                    jnp.zeros((CHIPS, 1, WIDTH), F32)], axis=1)

        ex_own, ex_got = extra_rows(0), core_swap(extra_rows(1))
        _, ex_in = stage2(ex_own, ex_got, 0)
        _, ex_part = stage3(ex_own, ex_got, 0, ex_in[0])
        extra = finish(ex_own, ex_got, 0, ex_in[1], ex_part)
        b_row = extra[6].astype(BF16)
        return (y_out, grad_x, extra[0], extra[1], unrow(grad_qkv[0]), b_row[:QROWS].reshape(HEADS, HEAD_DIM),
                unrow(grad_qkv[1]), unrow(grad_qkv[2]), b_row[QROWS:2 * QROWS].reshape(HEADS, HEAD_DIM), grad_wo,
                extra[2].astype(BF16), extra[3], extra[4], grad_w1, b_row[2 * QROWS:2 * QROWS + MLP], grad_w2,
                extra[5].astype(BF16))

    return jax.shard_map(layer_step, mesh=mesh3, in_specs=in_specs, out_specs=out_specs, check_vma=False)
```

```python
import math
import jax
import jax.numpy as jnp
from jax import lax
from jax.experimental import pallas as pl
from jax.experimental.pallas import tpu as pltpu
from jax.sharding import Mesh, PartitionSpec as P

LN_EPS = 1e-6
BF16 = jnp.bfloat16
F32 = jnp.float32

CHIPS = 4
HEADS = 2
HEAD_DIM = 72
QROWS = HEADS * HEAD_DIM
WIDTH = 1152
MLP = 538
MLP_PAD = 544
HALF = MLP_PAD // 2
ALL_AXES = ('dp', 'chip', 'core')
N_HEADS = 16
WIN_LANES = 256
UNROLL_F = 16
UNROLL_B = 16
ATT_SCALE = 1.0 / math.sqrt(HEAD_DIM)


def layer_norm(rows, ln_gain, ln_bias):
    row_mean = jnp.mean(rows, axis=-1, keepdims=True)
    centered = rows - row_mean
    variance = jnp.mean(centered * centered, axis=-1, keepdims=True)
    return centered * lax.rsqrt(variance + LN_EPS) * ln_gain + ln_bias


def gelu_tanh(pre_act):
    return jax.nn.gelu(pre_act, approximate=True)


def dot_nt(a, b):
    return lax.dot_general(a, b, (((1,), (1,)), ((), ())), preferred_element_type=F32)


def dot_nn(a, b):
    return lax.dot_general(a, b, (((1,), (0,)), ((), ())), preferred_element_type=F32)


def dot_tn(a, b):
    return lax.dot_general(a, b, (((0,), (0,)), ((), ())), preferred_element_type=F32)


def head_window(head):
    low = head * HEAD_DIM
    base = jnp.minimum(low // 128, WIDTH // 128 - WIN_LANES // 128) * 128
    base = pl.multiple_of(base, 128)
    lane = lax.broadcasted_iota(jnp.int32, (1, WIN_LANES), 1)
    mask = (lane >= low - base) & (lane < low - base + HEAD_DIM)
    return base, mask


def head_rows(ref, base):
    val = ref[:, 0, :, pl.ds(base, WIN_LANES)]
    return val.reshape(val.shape[0] * val.shape[1], WIN_LANES)


def probs_t(keys, queries):
    scores = dot_nt(keys, queries) * ATT_SCALE
    scores = jnp.exp(scores - jnp.max(scores, axis=0, keepdims=True))
    return scores * (1.0 / jnp.sum(scores, axis=0, keepdims=True))


def attn_fwd(q_ref, k_ref, v_ref, out_ref, acc):
    acc[...] = jnp.zeros_like(acc)

    def body(head, _):
        base, mask = head_window(head)
        zero = jnp.zeros((), BF16)
        keys = jnp.where(mask, head_rows(k_ref, base), zero)
        vals = jnp.where(mask, head_rows(v_ref, base), zero)
        probs = probs_t(keys, head_rows(q_ref, base)).astype(BF16)
        acc[:, pl.ds(base, WIN_LANES)] += dot_tn(probs, vals)
        return 0

    lax.fori_loop(0, N_HEADS, body, 0, unroll=UNROLL_F)
    out_ref[...] = acc[...].astype(BF16).reshape(out_ref.shape)


def attn_bwd(q_ref, k_ref, v_ref, do_ref, out_ref, acc):
    acc[...] = jnp.zeros_like(acc)

    def body(head, _):
        base, mask = head_window(head)
        zero = jnp.zeros((), BF16)
        queries = jnp.where(mask, head_rows(q_ref, base), zero)
        keys = jnp.where(mask, head_rows(k_ref, base), zero)
        d_out = jnp.where(mask, head_rows(do_ref, base), zero)
        probs = probs_t(keys, queries)
        d_probs = dot_nt(head_rows(v_ref, base), d_out).astype(BF16).astype(F32)
        prod = d_probs * probs
        d_scores = (prod - probs * jnp.sum(prod, axis=0, keepdims=True)) * ATT_SCALE
        d_scores = d_scores.astype(BF16)
        acc[:, pl.ds(base, WIN_LANES)] += dot_tn(d_scores, keys)
        acc[:, pl.ds(pl.multiple_of(base + WIDTH, 128), WIN_LANES)] += dot_nn(d_scores, queries)
        acc[:, pl.ds(pl.multiple_of(base + 2 * WIDTH, 128), WIN_LANES)] += dot_nn(probs.astype(BF16), d_out)
        return 0

    lax.fori_loop(0, N_HEADS, body, 0, unroll=UNROLL_B)
    out_ref[...] = acc[...].astype(BF16).reshape(out_ref.shape)


def part_spec(groups, toks, part):
    return pl.BlockSpec((groups, 1, toks, WIDTH), lambda i: (0, i, 0, part))


def attention_cost(inputs, parts, out_parts, dots):
    groups, images, toks, _ = inputs[0].shape
    n_tok = groups * toks
    return pl.CostEstimate(flops=dots * 8 * images * n_tok * n_tok * WIN_LANES * N_HEADS,
                           bytes_accessed=images * n_tok * WIDTH * 2 * (len(parts) + out_parts),
                           transcendentals=images * n_tok * n_tok * N_HEADS)


def attention_call(body, inputs, parts, out_parts, dots):
    groups, images, toks, _ = inputs[0].shape
    return pl.pallas_call(
        body, grid=(images,),
        out_shape=jax.ShapeDtypeStruct((groups, images, toks, out_parts * WIDTH), BF16),
        in_specs=[part_spec(groups, toks, p) for p in parts],
        out_specs=pl.BlockSpec((groups, 1, toks, out_parts * WIDTH), lambda i: (0, i, 0, 0)),
        scratch_shapes=[pltpu.VMEM((groups * toks, out_parts * WIDTH), F32)],
        cost_estimate=attention_cost(inputs, parts, out_parts, dots))(*inputs)


def attention_forward(qkv):
    return attention_call(attn_fwd, (qkv,) * 3, (0, 1, 2), 1, 2)


def attention_backward(qkv, d_mixed):
    return attention_call(attn_bwd, (qkv,) * 3 + (d_mixed,), (0, 1, 2, 0), 3, 5)


def tie(val, *deps):
    return lax.optimization_barrier((val,) + deps)[0]


def solution(mesh):
    mesh3 = Mesh(mesh.devices.reshape(2, CHIPS, 2), ALL_AXES)
    tp = ('chip', 'core')
    act_spec = P('dp', tp, None)
    replicated = P()
    head_w = P(None, tp, None)
    head_b = P(tp, None)
    grad_head_w = P('dp', tp, None)
    dp_tp = ('dp', 'chip', 'core')
    grad_head_b = P(dp_tp, None)
    grad_vec = P('dp')
    in_specs = (act_spec, act_spec, replicated, replicated, head_w, head_b, head_w, head_w, head_b,
                P(tp, None, None), replicated, replicated, replicated, P(None, tp), P(tp), P(tp, None), replicated)
    out_specs = (act_spec, act_spec, grad_vec, grad_vec, grad_head_w, grad_head_b, grad_head_w, grad_head_w, grad_head_b,
                 P(dp_tp, None, None), grad_vec, grad_vec, grad_vec, P('dp', tp), P(dp_tp),
                 P(dp_tp, None), grad_vec)

    def tp_perm(fn):
        return [(i, fn(i)) for i in range(8)]

    def permute(val, fn):
        return lax.ppermute(val, tp, tp_perm(fn))

    def core_swap(val):
        return permute(val, lambda i: i ^ 1)

    def pick(val, idx, axis=0):
        return lax.dynamic_index_in_dim(val, idx, axis, keepdims=False)

    def layer_step(x, d_out, ln1_gain, ln1_bias, w_q, b_q, w_k, w_v, b_v, w_o, b_o, ln2_gain, ln2_bias, w_1, b_1, w_2, b_2):
        dp = lax.axis_index('dp')
        chip = lax.axis_index('chip')
        core = lax.axis_index('core')
        cx, cy = chip % 2, chip // 2
        core0 = core == 0
        images = x.shape[0] // 8
        toks = x.shape[1]
        rows = images * toks * 8

        first = lambda i: (i ^ 2) if i % 2 == 0 else (i ^ 4)
        second = lambda i: (i ^ 4) if i % 2 == 0 else (i ^ 2)
        me = jnp.where(core0, cy, cx)
        away = lambda k: jnp.where(core0, k * 2 + (1 - cx), (1 - cy) * 2 + k)
        near = lambda k: jnp.where(core0, k * 2 + cx, cy * 2 + k)

        def stage2(own, got, axis):
            blk = lambda i: pick(own, i, axis) + pick(got, i, axis)
            send = (blk(away(1 - me)), blk(away(me)))
            far = permute(send[0], first)
            close = permute(send[1], first)
            return send, (far, close)

        def stage3(own, got, axis, far):
            send = pick(own, near(1 - me), axis) + pick(got, near(1 - me), axis) + far
            return send, permute(send, second)

        def finish(own, got, axis, close, part):
            return pick(own, near(me), axis) + pick(got, near(me), axis) + close + part

        def gather_all(half0, half1):
            return lax.all_gather(jnp.where(dp == 0, half0, half1), ALL_AXES, axis=0, tiled=False).reshape(2, 8, *half0.shape)

        def gather_own(half0, half1):
            own = lax.all_gather(jnp.where(dp == 0, half0, half1), ('dp', 'chip'), axis=0, tiled=False)
            return own.reshape(2 * CHIPS * HALF, WIDTH)

        def swap_weights(own):
            return [own, core_swap(own)]

        def rows_of(w):
            return jnp.transpose(w, (1, 2, 0)).reshape(QROWS, WIDTH)

        b1_pad = jnp.pad(b_1, (0, MLP_PAD - MLP))

        def bias_rows(head_bias, mlp_bias):
            row = jnp.concatenate([head_bias.reshape(QROWS), mlp_bias])
            return jnp.pad(row[None], ((0, 15), (0, WIDTH - row.shape[0])))

        att0 = jnp.concatenate([rows_of(w_q), rows_of(w_k), bias_rows(b_q, b1_pad[:HALF])])
        att1 = jnp.concatenate([rows_of(w_v), w_o.reshape(QROWS, WIDTH), bias_rows(b_v, b1_pad[HALF:])])
        att = gather_all(att0, att1)
        w1_rows = jnp.pad(w_1.T, ((0, MLP_PAD - MLP), (0, 0)))
        w2_rows = jnp.pad(w_2, ((0, MLP_PAD - MLP), (0, 0)))
        w1_all = swap_weights(gather_own(w1_rows[:HALF], w1_rows[HALF:]))
        w2_own_rows = gather_own(w2_rows[:HALF], w2_rows[HALF:])

        flat = CHIPS * QROWS
        part = lambda half, first: att[half, :, first:first + QROWS].reshape(2 * flat, WIDTH)
        bias = lambda half: att[half, :, 2 * QROWS, :QROWS].reshape(2 * flat)
        wqkv = jnp.concatenate([part(0, 0), part(0, QROWS), part(1, 0)])
        wo_all = part(1, QROWS)
        bqkv = jnp.concatenate([bias(0), jnp.zeros((2 * flat,), BF16), bias(1)]).astype(F32)
        b1_rows = att[:, :, 2 * QROWS, QROWS:QROWS + HALF].reshape(2, CHIPS, 2, HALF)
        b1_all = [pick(b1_rows, c, 2).reshape(2 * CHIPS * HALF).astype(F32) for c in (core, 1 - core)]

        x_rows = lax.all_to_all(x.reshape(8, images * toks, WIDTH), tp, 0, 0).reshape(rows, WIDTH)
        x_f32 = x_rows.astype(F32)
        h_one_f, ln1_pull = jax.vjp(layer_norm, x_f32, ln1_gain, ln1_bias)
        h_one = h_one_f.astype(BF16)
        qkv = (dot_nt(h_one, wqkv) + bqkv).astype(BF16)
        qkv = qkv.reshape(8, images, toks, 3 * WIDTH)
        mixed = attention_forward(qkv).reshape(rows, WIDTH)
        g_out = tie(d_out.reshape(8, images * toks, WIDTH), mixed)
        g_out = lax.all_to_all(g_out, tp, 0, 0).reshape(rows, WIDTH)
        attn_out = dot_nn(mixed, wo_all)
        x_mid = (x_f32 + attn_out + b_o).astype(BF16)
        mid_f32 = x_mid.astype(F32)
        h_two_f, ln2_pull = jax.vjp(layer_norm, mid_f32, ln2_gain, ln2_bias)
        h_two = h_two_f.astype(BF16)
        blocks = (2, CHIPS, HALF, WIDTH)
        hidden, gelu_pulls = [], []
        for w1, b1 in zip(w1_all, b1_all):
            pre_act = dot_nt(tie(h_two, *hidden), w1)
            pre_act = (pre_act + b1).astype(BF16)
            hid_f, gelu_pull = jax.vjp(gelu_tanh, pre_act.astype(F32))
            hidden.append(hid_f.astype(BF16))
            gelu_pulls.append(gelu_pull)
        w2_oth = dot_tn(hidden[1], g_out).reshape(blocks)
        w2_got = core_swap(w2_oth)
        w2_own = dot_tn(tie(hidden[0], w2_oth), g_out).reshape(blocks)
        w2_all = swap_weights(tie(w2_own_rows, w2_own))
        w2_send, w2_in = stage2(w2_own, w2_got, 1)
        g_mlp = tie(g_out, *w2_send)
        d_pre = [None, None]
        for c in (0, 1):
            d_hidden = dot_nt(tie(g_mlp, *d_pre[:c]), w2_all[c]).astype(BF16)
            (d_pre_f,) = gelu_pulls[c](d_hidden.astype(F32))
            d_pre[c] = d_pre_f.astype(BF16)
        w1_oth = dot_tn(d_pre[1], h_two).reshape(blocks)
        w1_got = core_swap(w1_oth)
        w1_own = dot_tn(tie(d_pre[0], w1_oth), h_two).reshape(blocks)
        w1_send, w1_in = stage2(w1_own, w1_got, 1)
        d_pre_t = [tie(d, *w1_send) for d in d_pre]
        d_h_two = (dot_nn(d_pre_t[0], w1_all[0]) + dot_nn(d_pre_t[1], w1_all[1])).astype(BF16)
        d_mid_ln, g_ln2_gain, g_ln2_bias = ln2_pull(d_h_two.astype(F32))
        d_mid = (g_out.astype(F32) + d_mid_ln).astype(BF16)
        d_mixed = dot_nt(d_mid, wo_all).astype(BF16)
        dw_o = dot_tn(mixed, d_mid).reshape(CHIPS, 2, QROWS, WIDTH)
        wo_own, wo_oth = pick(dw_o, core, 1), pick(dw_o, 1 - core, 1)
        wo_got = core_swap(wo_oth)
        w2_last, w2_part = stage3(w2_own, w2_got, 1, w2_in[0])
        mlp_out = dot_nn(tie(hidden[0], d_mixed), w2_all[0])
        mlp_out = mlp_out + dot_nn(hidden[1], w2_all[1])
        y_rows = (mid_f32 + mlp_out + b_2).astype(BF16)
        d_mixed = tie(d_mixed, w2_last).reshape(8, images, toks, WIDTH)
        d_qkv = attention_backward(qkv, d_mixed).reshape(rows, 3 * WIDTH)
        y_out = lax.all_to_all(y_rows.reshape(8, images * toks, WIDTH), tp, 0, 0).reshape(x.shape)
        w1_last, w1_part = stage3(w1_own, w1_got, 1, w1_in[0])
        d_qkv = tie(d_qkv, w1_last)
        own, got, sends, ins = {}, {}, {}, {}
        for n, name in enumerate('qkv'):
            dw = dot_tn(d_qkv[:, n * WIDTH:(n + 1) * WIDTH], h_one).reshape(CHIPS, 2, QROWS, WIDTH)
            own[name], oth = pick(dw, core, 1), pick(dw, 1 - core, 1)
            got[name] = core_swap(oth)
            d_qkv = tie(d_qkv, oth)
        sends['q'], ins['q'] = stage2(own['q'], got['q'], 0)
        wo_send, wo_in = stage2(wo_own, wo_got, 0)
        d_h_one = dot_nn(tie(d_qkv, *sends['q'], *wo_send), wqkv).astype(BF16)
        for name in 'kv':
            sends[name], ins[name] = stage2(own[name], got[name], 0)
        d_h_one = tie(d_h_one, *sends['k'], *sends['v'])
        d_in_ln, g_ln1_gain, g_ln1_bias = ln1_pull(d_h_one.astype(F32))
        g_x = (d_mid.astype(F32) + d_in_ln).astype(BF16)
        grad_x = lax.all_to_all(g_x.reshape(8, images * toks, WIDTH), tp, 0, 0).reshape(x.shape)
        _, wo_part = stage3(wo_own, wo_got, 0, wo_in[0])
        grad_qkv = {}
        for name in 'qkv':
            _, last = stage3(own[name], got[name], 0, ins[name][0])
            grad_qkv[name] = finish(own[name], got[name], 0, ins[name][1], last).astype(BF16)

        grad_w2 = finish(w2_own, w2_got, 1, w2_in[1], w2_part)
        grad_w2 = grad_w2.reshape(MLP_PAD, WIDTH)[:MLP].astype(BF16)
        grad_w1 = finish(w1_own, w1_got, 1, w1_in[1], w1_part)
        grad_w1 = grad_w1.reshape(MLP_PAD, WIDTH)[:MLP].T.astype(BF16)
        grad_wo = finish(wo_own, wo_got, 0, wo_in[1], wo_part)
        grad_wo = grad_wo.reshape(HEADS, HEAD_DIM, WIDTH).astype(BF16)
        unrow = lambda w: jnp.transpose(w.reshape(HEADS, HEAD_DIM, WIDTH), (2, 0, 1))

        col_sum = lambda v: jnp.sum(v, axis=0, dtype=F32)
        vecs = jnp.stack([g_ln1_gain, g_ln1_bias, col_sum(d_mid), g_ln2_gain, g_ln2_bias, col_sum(g_out)])

        qkv_sums = col_sum(d_qkv).reshape(3, CHIPS, 2, QROWS)

        def extra_rows(c):
            sums = pick(qkv_sums, core if c == 0 else 1 - core, 2)
            b1_sum = jnp.transpose(col_sum(d_pre[c]).reshape(2, CHIPS, HALF), (1, 0, 2)).reshape(CHIPS, MLP_PAD)
            row = jnp.concatenate([sums[0], sums[2], b1_sum, jnp.zeros((CHIPS, WIDTH - 2 * QROWS - MLP_PAD), F32)], axis=1)
            return jnp.concatenate([jnp.broadcast_to(vecs, (CHIPS, 6, WIDTH)), row[:, None],
                                    jnp.zeros((CHIPS, 1, WIDTH), F32)], axis=1)

        ex_own, ex_got = extra_rows(0), core_swap(extra_rows(1))
        _, ex_in = stage2(ex_own, ex_got, 0)
        _, ex_part = stage3(ex_own, ex_got, 0, ex_in[0])
        extra = finish(ex_own, ex_got, 0, ex_in[1], ex_part)
        b_row = extra[6].astype(BF16)
        return (y_out, grad_x, extra[0], extra[1], unrow(grad_qkv['q']), b_row[:QROWS].reshape(HEADS, HEAD_DIM),
                unrow(grad_qkv['k']), unrow(grad_qkv['v']), b_row[QROWS:2 * QROWS].reshape(HEADS, HEAD_DIM), grad_wo,
                extra[2].astype(BF16), extra[3], extra[4], grad_w1, b_row[2 * QROWS:2 * QROWS + MLP], grad_w2,
                extra[5].astype(BF16))

    return jax.shard_map(layer_step, mesh=mesh3, in_specs=in_specs, out_specs=out_specs, check_vma=False)
```

```python
import math
import jax
import jax.numpy as jnp
from jax import lax
from jax.experimental import pallas as pl
from jax.experimental.pallas import tpu as pltpu
from jax.sharding import Mesh, PartitionSpec as P

LN_EPS = 1e-6
BF16 = jnp.bfloat16
F32 = jnp.float32

CHIPS = 4
HEADS = 2
HEAD_DIM = 72
QROWS = HEADS * HEAD_DIM
WIDTH = 1152
MLP = 538
MLP_PAD = 544
HALF = MLP_PAD // 2
ALL_AXES = ('dp', 'chip', 'core')
N_HEADS = 16
WIN_LANES = 256
GRAD_COLS = 384
UNROLL_F = 16
UNROLL_B = 16
ATT_SCALE = 1.0 / math.sqrt(HEAD_DIM)


def layer_norm(rows, ln_gain, ln_bias):
    row_mean = jnp.mean(rows, axis=-1, keepdims=True)
    centered = rows - row_mean
    variance = jnp.mean(centered * centered, axis=-1, keepdims=True)
    return centered * lax.rsqrt(variance + LN_EPS) * ln_gain + ln_bias


def gelu_tanh(pre_act):
    return jax.nn.gelu(pre_act, approximate=True)


def dot_nt(a, b):
    return lax.dot_general(a, b, (((1,), (1,)), ((), ())), preferred_element_type=F32)


def dot_nn(a, b):
    return lax.dot_general(a, b, (((1,), (0,)), ((), ())), preferred_element_type=F32)


def dot_tn(a, b):
    return lax.dot_general(a, b, (((0,), (0,)), ((), ())), preferred_element_type=F32)


def head_window(head):
    low = head * HEAD_DIM
    base = jnp.minimum(low // 128, WIDTH // 128 - WIN_LANES // 128) * 128
    base = pl.multiple_of(base, 128)
    lane = lax.broadcasted_iota(jnp.int32, (1, WIN_LANES), 1)
    mask = (lane >= low - base) & (lane < low - base + HEAD_DIM)
    return base, mask


def head_rows(ref, base):
    val = ref[:, 0, :, pl.ds(base, WIN_LANES)]
    return val.reshape(val.shape[0] * val.shape[1], WIN_LANES)


def probs_t(keys, queries):
    scores = dot_nt(keys, queries) * ATT_SCALE
    scores = jnp.exp(scores - jnp.max(scores, axis=0, keepdims=True))
    return scores * (1.0 / jnp.sum(scores, axis=0, keepdims=True))


def attn_fwd(q_ref, k_ref, v_ref, out_ref, acc):
    acc[...] = jnp.zeros_like(acc)

    def body(head, _):
        base, mask = head_window(head)
        zero = jnp.zeros((), BF16)
        keys = jnp.where(mask, head_rows(k_ref, base), zero)
        vals = jnp.where(mask, head_rows(v_ref, base), zero)
        probs = probs_t(keys, head_rows(q_ref, base)).astype(BF16)
        acc[:, pl.ds(base, WIN_LANES)] += dot_tn(probs, vals)
        return 0

    lax.fori_loop(0, N_HEADS, body, 0, unroll=UNROLL_F)
    out_ref[...] = acc[...].astype(BF16).reshape(out_ref.shape)


def attn_bwd(q_ref, k_ref, v_ref, do_ref, out_ref, acc):
    acc[...] = jnp.zeros_like(acc)

    def body(head, _):
        base, mask = head_window(head)
        zero = jnp.zeros((), BF16)
        queries = jnp.where(mask, head_rows(q_ref, base), zero)
        keys = jnp.where(mask, head_rows(k_ref, base), zero)
        d_out = jnp.where(mask, head_rows(do_ref, base), zero)
        probs = probs_t(keys, queries)
        d_probs = dot_nt(head_rows(v_ref, base), d_out).astype(BF16).astype(F32)
        prod = d_probs * probs
        d_scores = (prod - probs * jnp.sum(prod, axis=0, keepdims=True)) * ATT_SCALE
        d_scores = d_scores.astype(BF16)
        acc[:, pl.ds(base, WIN_LANES)] += dot_tn(d_scores, keys)
        acc[:, pl.ds(pl.multiple_of(base + WIDTH, 128), WIN_LANES)] += dot_nn(d_scores, queries)
        acc[:, pl.ds(pl.multiple_of(base + 2 * WIDTH, 128), WIN_LANES)] += dot_nn(probs.astype(BF16), d_out)
        return 0

    lax.fori_loop(0, N_HEADS, body, 0, unroll=UNROLL_B)
    out_ref[...] = acc[...].astype(BF16).reshape(out_ref.shape)


def part_spec(groups, toks, part):
    return pl.BlockSpec((groups, 1, toks, WIDTH), lambda i: (0, i, 0, part))


def attention_cost(inputs, parts, out_parts, dots):
    groups, images, toks, _ = inputs[0].shape
    n_tok = groups * toks
    return pl.CostEstimate(flops=dots * 8 * images * n_tok * n_tok * WIN_LANES * N_HEADS,
                           bytes_accessed=images * n_tok * WIDTH * 2 * (len(parts) + out_parts),
                           transcendentals=images * n_tok * n_tok * N_HEADS)


def attention_call(body, inputs, parts, out_parts, dots):
    groups, images, toks, _ = inputs[0].shape
    return pl.pallas_call(
        body, grid=(images,),
        out_shape=jax.ShapeDtypeStruct((groups, images, toks, out_parts * WIDTH), BF16),
        in_specs=[part_spec(groups, toks, p) for p in parts],
        out_specs=pl.BlockSpec((groups, 1, toks, out_parts * WIDTH), lambda i: (0, i, 0, 0)),
        scratch_shapes=[pltpu.VMEM((groups * toks, out_parts * WIDTH), F32)],
        cost_estimate=attention_cost(inputs, parts, out_parts, dots))(*inputs)


def attention_forward(qkv):
    return attention_call(attn_fwd, (qkv,) * 3, (0, 1, 2), 1, 2)


def attention_backward(qkv, d_mixed):
    return attention_call(attn_bwd, (qkv,) * 3 + (d_mixed,), (0, 1, 2, 0), 3, 5)


def qkv_grads(d_ref, h_ref, w_ref, dw_ref, dh_ref, sum_ref, acc):
    step = pl.program_id(0)
    d_cols = d_ref[...]
    dw_ref[...] = dot_tn(d_cols, h_ref[...])
    sum_ref[...] = jnp.sum(d_cols.astype(F32), axis=0, keepdims=True)
    part = dot_nn(d_cols, w_ref[...])

    @pl.when(step == 0)
    def _():
        acc[...] = part

    @pl.when(step > 0)
    def _():
        acc[...] += part

    @pl.when(step == pl.num_programs(0) - 1)
    def _():
        dh_ref[...] = acc[...].astype(BF16)


def projection_backward(d_qkv, h_one, wqkv):
    rows, cols = d_qkv.shape
    block = GRAD_COLS
    whole = pl.BlockSpec((rows, WIDTH), lambda j: (0, 0))
    piece = pl.BlockSpec((block, WIDTH), lambda j: (j, 0))
    return pl.pallas_call(
        qkv_grads, grid=(cols // block,), name='qkv_grads',
        out_shape=(jax.ShapeDtypeStruct((cols, WIDTH), F32), jax.ShapeDtypeStruct((rows, WIDTH), BF16), jax.ShapeDtypeStruct((1, cols), F32)),
        in_specs=[pl.BlockSpec((rows, block), lambda j: (0, j)), whole, piece],
        out_specs=(piece, whole, pl.BlockSpec((1, block), lambda j: (0, j))),
        scratch_shapes=[pltpu.VMEM((rows, WIDTH), F32)],
        cost_estimate=pl.CostEstimate(flops=8 * rows * cols * WIDTH, bytes_accessed=cols * WIDTH * 6 + rows * cols * 2, transcendentals=0),
    )(d_qkv, h_one, wqkv)


def tie(val, *deps):
    return lax.optimization_barrier((val,) + deps)[0]


def solution(mesh):
    mesh3 = Mesh(mesh.devices.reshape(2, CHIPS, 2), ALL_AXES)
    tp = ('chip', 'core')
    act_spec = P('dp', tp, None)
    replicated = P()
    head_w = P(None, tp, None)
    head_b = P(tp, None)
    grad_head_w = P('dp', tp, None)
    dp_tp = ('dp', 'chip', 'core')
    grad_head_b = P(dp_tp, None)
    grad_vec = P('dp')
    in_specs = (act_spec, act_spec, replicated, replicated, head_w, head_b, head_w, head_w, head_b,
                P(tp, None, None), replicated, replicated, replicated, P(None, tp), P(tp), P(tp, None), replicated)
    out_specs = (act_spec, act_spec, grad_vec, grad_vec, grad_head_w, grad_head_b, grad_head_w, grad_head_w, grad_head_b,
                 P(dp_tp, None, None), grad_vec, grad_vec, grad_vec, P('dp', tp), P(dp_tp),
                 P(dp_tp, None), grad_vec)

    def tp_perm(fn):
        return [(i, fn(i)) for i in range(8)]

    def permute(val, fn):
        return lax.ppermute(val, tp, tp_perm(fn))

    def core_swap(val):
        return permute(val, lambda i: i ^ 1)

    def pick(val, idx, axis=0):
        return lax.dynamic_index_in_dim(val, idx, axis, keepdims=False)

    def layer_step(x, d_out, ln1_gain, ln1_bias, w_q, b_q, w_k, w_v, b_v, w_o, b_o, ln2_gain, ln2_bias, w_1, b_1, w_2, b_2):
        dp = lax.axis_index('dp')
        chip = lax.axis_index('chip')
        core = lax.axis_index('core')
        cx, cy = chip % 2, chip // 2
        core0 = core == 0
        images = x.shape[0] // 8
        toks = x.shape[1]
        rows = images * toks * 8

        first = lambda i: (i ^ 2) if i % 2 == 0 else (i ^ 4)
        second = lambda i: (i ^ 4) if i % 2 == 0 else (i ^ 2)
        me = jnp.where(core0, cy, cx)
        away = lambda k: jnp.where(core0, k * 2 + (1 - cx), (1 - cy) * 2 + k)
        near = lambda k: jnp.where(core0, k * 2 + cx, cy * 2 + k)

        def chip_sums(own, got, axis):
            return lambda i: pick(own, i, axis) + pick(got, i, axis)

        def stage2(blk):
            send = lax.optimization_barrier((blk(away(1 - me)), blk(away(me))))
            far = permute(send[0], first)
            close = permute(send[1], first)
            return send, (far, close)

        def stage3(blk, far):
            send = lax.optimization_barrier(blk(near(1 - me)) + far)
            return send, permute(send, second)

        def finish(blk, close, part):
            return blk(near(me)) + close + part

        def gather_all(half0, half1):
            return lax.all_gather(jnp.where(dp == 0, half0, half1), ALL_AXES, axis=0, tiled=False).reshape(2, 8, *half0.shape)

        def gather_own(half0, half1):
            own = lax.all_gather(jnp.where(dp == 0, half0, half1), ('dp', 'chip'), axis=0, tiled=False)
            return own.reshape(2 * CHIPS * HALF, WIDTH)

        def swap_weights(own):
            return [own, core_swap(own)]

        def rows_of(w):
            return jnp.transpose(w, (1, 2, 0)).reshape(QROWS, WIDTH)

        b1_pad = jnp.pad(b_1, (0, MLP_PAD - MLP))

        def bias_rows(head_bias, mlp_bias):
            row = jnp.concatenate([head_bias.reshape(QROWS), mlp_bias])
            return jnp.pad(row[None], ((0, 15), (0, WIDTH - row.shape[0])))

        att0 = jnp.concatenate([rows_of(w_q), rows_of(w_k), bias_rows(b_q, b1_pad[:HALF])])
        att1 = jnp.concatenate([rows_of(w_v), w_o.reshape(QROWS, WIDTH), bias_rows(b_v, b1_pad[HALF:])])
        att = gather_all(att0, att1)
        w1_rows = jnp.pad(w_1.T, ((0, MLP_PAD - MLP), (0, 0)))
        w2_rows = jnp.pad(w_2, ((0, MLP_PAD - MLP), (0, 0)))
        w1_all = swap_weights(gather_own(w1_rows[:HALF], w1_rows[HALF:]))
        w2_own_rows = gather_own(w2_rows[:HALF], w2_rows[HALF:])

        flat = CHIPS * QROWS
        part = lambda half, first: att[half, :, first:first + QROWS].reshape(2 * flat, WIDTH)
        bias = lambda half: att[half, :, 2 * QROWS, :QROWS].reshape(2 * flat)
        wqkv = jnp.concatenate([part(0, 0), part(0, QROWS), part(1, 0)])
        wo_all = part(1, QROWS)
        bqkv = jnp.concatenate([bias(0), jnp.zeros((2 * flat,), BF16), bias(1)]).astype(F32)
        b1_rows = att[:, :, 2 * QROWS, QROWS:QROWS + HALF].reshape(2, CHIPS, 2, HALF)
        b1_all = [pick(b1_rows, c, 2).reshape(2 * CHIPS * HALF).astype(F32) for c in (core, 1 - core)]

        x_rows = lax.all_to_all(x.reshape(8, images * toks, WIDTH), tp, 0, 0).reshape(rows, WIDTH)
        x_f32 = x_rows.astype(F32)
        h_one_f, ln1_pull = jax.vjp(layer_norm, x_f32, ln1_gain, ln1_bias)
        h_one = h_one_f.astype(BF16)
        qkv = (dot_nt(h_one, wqkv) + bqkv).astype(BF16)
        qkv = qkv.reshape(8, images, toks, 3 * WIDTH)
        mixed = attention_forward(qkv).reshape(rows, WIDTH)
        g_out = tie(d_out.reshape(8, images * toks, WIDTH), mixed)
        g_out = lax.all_to_all(g_out, tp, 0, 0).reshape(rows, WIDTH)
        attn_out = dot_nn(mixed, wo_all)
        x_mid = (x_f32 + attn_out + b_o).astype(BF16)
        mid_f32 = x_mid.astype(F32)
        h_two_f, ln2_pull = jax.vjp(layer_norm, mid_f32, ln2_gain, ln2_bias)
        h_two = h_two_f.astype(BF16)
        blocks = (2, CHIPS, HALF, WIDTH)
        hidden, gelu_pulls = [], []
        for w1, b1 in zip(w1_all, b1_all):
            pre_act = dot_nt(tie(h_two, *hidden), w1)
            pre_act = (pre_act + b1).astype(BF16)
            hid_f, gelu_pull = jax.vjp(gelu_tanh, pre_act.astype(F32))
            hidden.append(hid_f.astype(BF16))
            gelu_pulls.append(gelu_pull)
        w2_oth = dot_tn(hidden[1], g_out).reshape(blocks)
        w2_got = core_swap(w2_oth)
        w2_own = dot_tn(tie(hidden[0], w2_oth), g_out).reshape(blocks)
        w2_all = swap_weights(tie(w2_own_rows, w2_own))
        w2_blk = chip_sums(w2_own, w2_got, 1)
        w2_send, w2_in = stage2(w2_blk)
        g_mlp = tie(g_out, *w2_send)
        d_pre = [None, None]
        for c in (0, 1):
            d_hidden = dot_nt(tie(g_mlp, *d_pre[:c]), w2_all[c]).astype(BF16)
            (d_pre_f,) = gelu_pulls[c](d_hidden.astype(F32))
            d_pre[c] = d_pre_f.astype(BF16)
        w1_oth = dot_tn(d_pre[1], h_two).reshape(blocks)
        w1_got = core_swap(w1_oth)
        w1_own = dot_tn(tie(d_pre[0], w1_oth), h_two).reshape(blocks)
        w1_blk = chip_sums(w1_own, w1_got, 1)
        w1_send, w1_in = stage2(w1_blk)
        d_pre_t = [tie(d, *w1_send) for d in d_pre]
        d_h_two = (dot_nn(d_pre_t[0], w1_all[0]) + dot_nn(d_pre_t[1], w1_all[1])).astype(BF16)
        d_mid_ln, g_ln2_gain, g_ln2_bias = ln2_pull(d_h_two.astype(F32))
        d_mid = (g_out.astype(F32) + d_mid_ln).astype(BF16)
        d_mixed = dot_nt(d_mid, wo_all).astype(BF16)
        dw_o = dot_tn(mixed, d_mid).reshape(CHIPS, 2, QROWS, WIDTH)
        wo_own, wo_oth = pick(dw_o, core, 1), pick(dw_o, 1 - core, 1)
        wo_got = core_swap(wo_oth)
        w2_last, w2_part = stage3(w2_blk, w2_in[0])
        mlp_out = dot_nn(tie(hidden[0], d_mixed), w2_all[0])
        mlp_out = mlp_out + dot_nn(hidden[1], w2_all[1])
        y_rows = (mid_f32 + mlp_out + b_2).astype(BF16)
        d_mixed = tie(d_mixed, w2_last).reshape(8, images, toks, WIDTH)
        d_qkv = attention_backward(qkv, d_mixed).reshape(rows, 3 * WIDTH)
        y_out = lax.all_to_all(y_rows.reshape(8, images * toks, WIDTH), tp, 0, 0).reshape(x.shape)
        w1_last, w1_part = stage3(w1_blk, w1_in[0])
        d_qkv = tie(d_qkv, w1_last)
        wo_blk = chip_sums(wo_own, wo_got, 0)
        wo_send, wo_in = stage2(wo_blk)
        dw_qkv, d_h_one, qkv_sums = projection_backward(tie(d_qkv, *wo_send), h_one, wqkv)
        dw_qkv = dw_qkv.reshape(3, CHIPS, 2, QROWS, WIDTH)
        qkv_own, qkv_oth = pick(dw_qkv, core, 2), pick(dw_qkv, 1 - core, 2)
        qkv_got = core_swap(qkv_oth)
        d_h_one = tie(d_h_one, qkv_oth)
        d_in_ln, g_ln1_gain, g_ln1_bias = ln1_pull(d_h_one.astype(F32))
        g_x = (d_mid.astype(F32) + d_in_ln).astype(BF16)
        col_sum = lambda v: jnp.sum(v, axis=0, dtype=F32)
        vecs = jnp.stack([g_ln1_gain, g_ln1_bias, col_sum(d_mid), g_ln2_gain, g_ln2_bias, col_sum(g_out)])
        head_sums = qkv_sums.reshape(3, CHIPS, 2, QROWS)
        mlp_sums = [jnp.transpose(col_sum(d).reshape(2, CHIPS, HALF), (1, 0, 2)).reshape(CHIPS, MLP_PAD) for d in d_pre]
        mlp_sums = jnp.where(core0, jnp.stack(mlp_sums, 1), jnp.stack(mlp_sums[::-1], 1))
        bias_sums = jnp.concatenate([head_sums[0], head_sums[2], mlp_sums, jnp.zeros((CHIPS, 2, WIDTH - 2 * QROWS - MLP_PAD), F32)], axis=2)
        small = jnp.concatenate([jnp.broadcast_to(vecs, (CHIPS, 6, WIDTH)), bias_sums], axis=1)
        qkv_sum = chip_sums(qkv_own, qkv_got, 1)
        qkv_blk = lambda i: jnp.concatenate([qkv_sum(i).reshape(3 * QROWS, WIDTH), pick(small, i)])
        _, qkv_in = stage2(qkv_blk)
        grad_x = lax.all_to_all(g_x.reshape(8, images * toks, WIDTH), tp, 0, 0).reshape(x.shape)
        _, wo_part = stage3(wo_blk, wo_in[0])
        _, qkv_part = stage3(qkv_blk, qkv_in[0])
        qkv_all = finish(qkv_blk, qkv_in[1], qkv_part)
        grad_qkv = qkv_all[:3 * QROWS].reshape(3, QROWS, WIDTH).astype(BF16)
        small_own = qkv_all[3 * QROWS:]
        extra = small_own + core_swap(small_own)
        b_row = pick(extra[6:], core).astype(BF16)

        grad_w2 = finish(w2_blk, w2_in[1], w2_part)
        grad_w2 = grad_w2.reshape(MLP_PAD, WIDTH)[:MLP].astype(BF16)
        grad_w1 = finish(w1_blk, w1_in[1], w1_part)
        grad_w1 = grad_w1.reshape(MLP_PAD, WIDTH)[:MLP].T.astype(BF16)
        grad_wo = finish(wo_blk, wo_in[1], wo_part)
        grad_wo = grad_wo.reshape(HEADS, HEAD_DIM, WIDTH).astype(BF16)
        unrow = lambda w: jnp.transpose(w.reshape(HEADS, HEAD_DIM, WIDTH), (2, 0, 1))

        return (y_out, grad_x, extra[0], extra[1], unrow(grad_qkv[0]), b_row[:QROWS].reshape(HEADS, HEAD_DIM),
                unrow(grad_qkv[1]), unrow(grad_qkv[2]), b_row[QROWS:2 * QROWS].reshape(HEADS, HEAD_DIM), grad_wo,
                extra[2].astype(BF16), extra[3], extra[4], grad_w1, b_row[2 * QROWS:2 * QROWS + MLP], grad_w2,
                extra[5].astype(BF16))

    return jax.shard_map(layer_step, mesh=mesh3, in_specs=in_specs, out_specs=out_specs, check_vma=False)
```

```python
import math
import jax
import jax.numpy as jnp
from jax import lax
from jax.experimental import pallas as pl
from jax.experimental.pallas import tpu as pltpu
from jax.sharding import Mesh, PartitionSpec as P

LN_EPS = 1e-6
BF16 = jnp.bfloat16
F32 = jnp.float32

CHIPS = 4
HEADS = 2
HEAD_DIM = 72
QROWS = HEADS * HEAD_DIM
WIDTH = 1152
MLP = 538
MLP_PAD = 544
HALF = MLP_PAD // 2
ALL_AXES = ('dp', 'chip', 'core')
N_HEADS = 16
WIN_LANES = 256
GRAD_COLS = 384
UNROLL_F = 16
UNROLL_B = 16
ATT_SCALE = 1.0 / math.sqrt(HEAD_DIM)


def layer_norm(rows, ln_gain, ln_bias):
    row_mean = jnp.mean(rows, axis=-1, keepdims=True)
    centered = rows - row_mean
    variance = jnp.mean(centered * centered, axis=-1, keepdims=True)
    return centered * lax.rsqrt(variance + LN_EPS) * ln_gain + ln_bias


def gelu_tanh(pre_act):
    return jax.nn.gelu(pre_act, approximate=True)


def dot_nt(a, b):
    return lax.dot_general(a, b, (((1,), (1,)), ((), ())), preferred_element_type=F32)


def dot_nn(a, b):
    return lax.dot_general(a, b, (((1,), (0,)), ((), ())), preferred_element_type=F32)


def dot_tn(a, b):
    return lax.dot_general(a, b, (((0,), (0,)), ((), ())), preferred_element_type=F32)


def head_window(head):
    low = head * HEAD_DIM
    base = jnp.minimum(low // 128, WIDTH // 128 - WIN_LANES // 128) * 128
    base = pl.multiple_of(base, 128)
    lane = lax.broadcasted_iota(jnp.int32, (1, WIN_LANES), 1)
    mask = (lane >= low - base) & (lane < low - base + HEAD_DIM)
    return base, mask


def head_rows(ref, base):
    val = ref[:, 0, :, pl.ds(base, WIN_LANES)]
    return val.reshape(val.shape[0] * val.shape[1], WIN_LANES)


def probs_t(keys, queries):
    scores = dot_nt(keys, queries) * ATT_SCALE
    scores = jnp.exp(scores - jnp.max(scores, axis=0, keepdims=True))
    return scores * (1.0 / jnp.sum(scores, axis=0, keepdims=True))


def attn_fwd(q_ref, k_ref, v_ref, out_ref, acc):
    acc[...] = jnp.zeros_like(acc)

    def body(head, _):
        base, mask = head_window(head)
        zero = jnp.zeros((), BF16)
        keys = jnp.where(mask, head_rows(k_ref, base), zero)
        vals = jnp.where(mask, head_rows(v_ref, base), zero)
        probs = probs_t(keys, head_rows(q_ref, base)).astype(BF16)
        acc[:, pl.ds(base, WIN_LANES)] += dot_tn(probs, vals)
        return 0

    lax.fori_loop(0, N_HEADS, body, 0, unroll=UNROLL_F)
    out_ref[...] = acc[...].astype(BF16).reshape(out_ref.shape)


def attn_bwd(q_ref, k_ref, v_ref, do_ref, out_ref, acc):
    acc[...] = jnp.zeros_like(acc)

    def body(head, _):
        base, mask = head_window(head)
        zero = jnp.zeros((), BF16)
        queries = jnp.where(mask, head_rows(q_ref, base), zero)
        keys = jnp.where(mask, head_rows(k_ref, base), zero)
        d_out = jnp.where(mask, head_rows(do_ref, base), zero)
        probs = probs_t(keys, queries)
        d_probs = dot_nt(head_rows(v_ref, base), d_out).astype(BF16).astype(F32)
        prod = d_probs * probs
        d_scores = (prod - probs * jnp.sum(prod, axis=0, keepdims=True)) * ATT_SCALE
        d_scores = d_scores.astype(BF16)
        acc[:, pl.ds(base, WIN_LANES)] += dot_tn(d_scores, keys)
        acc[:, pl.ds(pl.multiple_of(base + WIDTH, 128), WIN_LANES)] += dot_nn(d_scores, queries)
        acc[:, pl.ds(pl.multiple_of(base + 2 * WIDTH, 128), WIN_LANES)] += dot_nn(probs.astype(BF16), d_out)
        return 0

    lax.fori_loop(0, N_HEADS, body, 0, unroll=UNROLL_B)
    out_ref[...] = acc[...].astype(BF16).reshape(out_ref.shape)


def part_spec(groups, toks, part):
    return pl.BlockSpec((groups, 1, toks, WIDTH), lambda i: (0, i, 0, part))


def attention_cost(inputs, parts, out_parts, dots):
    groups, images, toks, _ = inputs[0].shape
    n_tok = groups * toks
    return pl.CostEstimate(flops=dots * 8 * images * n_tok * n_tok * WIN_LANES * N_HEADS,
                           bytes_accessed=images * n_tok * WIDTH * 2 * (len(parts) + out_parts),
                           transcendentals=images * n_tok * n_tok * N_HEADS)


def attention_call(body, inputs, parts, out_parts, dots):
    groups, images, toks, _ = inputs[0].shape
    return pl.pallas_call(
        body, grid=(images,),
        out_shape=jax.ShapeDtypeStruct((groups, images, toks, out_parts * WIDTH), BF16),
        in_specs=[part_spec(groups, toks, p) for p in parts],
        out_specs=pl.BlockSpec((groups, 1, toks, out_parts * WIDTH), lambda i: (0, i, 0, 0)),
        scratch_shapes=[pltpu.VMEM((groups * toks, out_parts * WIDTH), F32)],
        cost_estimate=attention_cost(inputs, parts, out_parts, dots))(*inputs)


def attention_forward(qkv):
    return attention_call(attn_fwd, (qkv,) * 3, (0, 1, 2), 1, 2)


def attention_backward(qkv, d_mixed):
    return attention_call(attn_bwd, (qkv,) * 3 + (d_mixed,), (0, 1, 2, 0), 3, 5)


def qkv_grads(d_ref, h_ref, w_ref, dw_ref, dh_ref, sum_ref, acc):
    step = pl.program_id(0)
    d_cols = d_ref[...]
    dw_ref[...] = dot_tn(d_cols, h_ref[...])
    sum_ref[...] = jnp.sum(d_cols.astype(F32), axis=0, keepdims=True)
    part = dot_nn(d_cols, w_ref[...])

    @pl.when(step == 0)
    def _():
        acc[...] = part

    @pl.when(step > 0)
    def _():
        acc[...] += part

    @pl.when(step == pl.num_programs(0) - 1)
    def _():
        dh_ref[...] = acc[...].astype(BF16)


def projection_backward(d_qkv, h_one, wqkv):
    rows, cols = d_qkv.shape
    block = GRAD_COLS
    whole = pl.BlockSpec((rows, WIDTH), lambda j: (0, 0))
    piece = pl.BlockSpec((block, WIDTH), lambda j: (j, 0))
    return pl.pallas_call(
        qkv_grads, grid=(cols // block,), name='qkv_grads',
        out_shape=(jax.ShapeDtypeStruct((cols, WIDTH), F32), jax.ShapeDtypeStruct((rows, WIDTH), BF16), jax.ShapeDtypeStruct((1, cols), F32)),
        in_specs=[pl.BlockSpec((rows, block), lambda j: (0, j)), whole, piece],
        out_specs=(piece, whole, pl.BlockSpec((1, block), lambda j: (0, j))),
        scratch_shapes=[pltpu.VMEM((rows, WIDTH), F32)],
        cost_estimate=pl.CostEstimate(flops=8 * rows * cols * WIDTH, bytes_accessed=cols * WIDTH * 6 + rows * cols * 2, transcendentals=0),
    )(d_qkv, h_one, wqkv)


def tie(val, *deps):
    return lax.optimization_barrier((val,) + deps)[0]


def solution(mesh):
    mesh3 = Mesh(mesh.devices.reshape(2, CHIPS, 2), ALL_AXES)
    tp = ('chip', 'core')
    act_spec = P('dp', tp, None)
    replicated = P()
    head_w = P(None, tp, None)
    head_b = P(tp, None)
    grad_head_w = P('dp', tp, None)
    dp_tp = ('dp', 'chip', 'core')
    grad_head_b = P(dp_tp, None)
    grad_vec = P('dp')
    in_specs = (act_spec, act_spec, replicated, replicated, head_w, head_b, head_w, head_w, head_b,
                P(tp, None, None), replicated, replicated, replicated, P(None, tp), P(tp), P(tp, None), replicated)
    out_specs = (act_spec, act_spec, grad_vec, grad_vec, grad_head_w, grad_head_b, grad_head_w, grad_head_w, grad_head_b,
                 P(dp_tp, None, None), grad_vec, grad_vec, grad_vec, P('dp', tp), P(dp_tp),
                 P(dp_tp, None), grad_vec)

    def tp_perm(fn):
        return [(i, fn(i)) for i in range(8)]

    def permute(val, fn):
        return lax.ppermute(val, tp, tp_perm(fn))

    def core_swap(val):
        return permute(val, lambda i: i ^ 1)

    def pick(val, idx, axis=0):
        return lax.dynamic_index_in_dim(val, idx, axis, keepdims=False)

    def layer_step(x, d_out, ln1_gain, ln1_bias, w_q, b_q, w_k, w_v, b_v, w_o, b_o, ln2_gain, ln2_bias, w_1, b_1, w_2, b_2):
        dp = lax.axis_index('dp')
        chip = lax.axis_index('chip')
        core = lax.axis_index('core')
        cx, cy = chip % 2, chip // 2
        core0 = core == 0
        images = x.shape[0] // 8
        toks = x.shape[1]
        rows = images * toks * 8

        first = lambda i: (i ^ 2) if i % 2 == 0 else (i ^ 4)
        second = lambda i: (i ^ 4) if i % 2 == 0 else (i ^ 2)
        me = jnp.where(core0, cy, cx)
        away = lambda k: jnp.where(core0, k * 2 + (1 - cx), (1 - cy) * 2 + k)
        near = lambda k: jnp.where(core0, k * 2 + cx, cy * 2 + k)

        def chip_sums(own, got, axis):
            return lambda i: pick(own, i, axis) + pick(got, i, axis)

        def stage2(blk):
            send = lax.optimization_barrier((blk(away(1 - me)), blk(away(me))))
            far = permute(send[0], first)
            close = permute(send[1], first)
            return send, (far, close)

        def stage3(blk, far):
            send = lax.optimization_barrier(blk(near(1 - me)) + far)
            return send, permute(send, second)

        def finish(blk, close, part):
            return blk(near(me)) + close + part

        def gather_all(half0, half1):
            return lax.all_gather(jnp.where(dp == 0, half0, half1), ALL_AXES, axis=0, tiled=False).reshape(2, 8, *half0.shape)

        def gather_own(half0, half1):
            own = lax.all_gather(jnp.where(dp == 0, half0, half1), ('dp', 'chip'), axis=0, tiled=False)
            return own.reshape(2 * CHIPS * HALF, WIDTH)

        def swap_weights(own):
            return [own, core_swap(own)]

        def rows_of(w):
            return jnp.transpose(w, (1, 2, 0)).reshape(QROWS, WIDTH)

        b1_pad = jnp.pad(b_1, (0, MLP_PAD - MLP))

        def bias_rows(head_bias, mlp_bias):
            row = jnp.concatenate([head_bias.reshape(QROWS), mlp_bias])
            return jnp.pad(row[None], ((0, 15), (0, WIDTH - row.shape[0])))

        att0 = jnp.concatenate([rows_of(w_q), rows_of(w_k), bias_rows(b_q, b1_pad[:HALF])])
        att1 = jnp.concatenate([rows_of(w_v), w_o.reshape(QROWS, WIDTH), bias_rows(b_v, b1_pad[HALF:])])
        att = gather_all(att0, att1)
        w1_rows = jnp.pad(w_1.T, ((0, MLP_PAD - MLP), (0, 0)))
        w2_rows = jnp.pad(w_2, ((0, MLP_PAD - MLP), (0, 0)))
        w1_own_rows = gather_own(w1_rows[:HALF], w1_rows[HALF:])
        w2_own_rows = gather_own(w2_rows[:HALF], w2_rows[HALF:])

        flat = CHIPS * QROWS
        part = lambda half, first: att[half, :, first:first + QROWS].reshape(2 * flat, WIDTH)
        bias = lambda half: att[half, :, 2 * QROWS, :QROWS].reshape(2 * flat)
        wqkv = jnp.concatenate([part(0, 0), part(0, QROWS), part(1, 0)])
        wo_all = part(1, QROWS)
        bqkv = jnp.concatenate([bias(0), jnp.zeros((2 * flat,), BF16), bias(1)]).astype(F32)
        b1_rows = att[:, :, 2 * QROWS, QROWS:QROWS + HALF].reshape(2, CHIPS, 2, HALF)
        b1_all = [pick(b1_rows, c, 2).reshape(2 * CHIPS * HALF).astype(F32) for c in (core, 1 - core)]

        x_rows = lax.all_to_all(x.reshape(8, images * toks, WIDTH), tp, 0, 0).reshape(rows, WIDTH)
        x_f32 = x_rows.astype(F32)
        h_one_f, ln1_pull = jax.vjp(layer_norm, x_f32, ln1_gain, ln1_bias)
        h_one = h_one_f.astype(BF16)
        qkv = (dot_nt(h_one, wqkv) + bqkv).astype(BF16)
        qkv = qkv.reshape(8, images, toks, 3 * WIDTH)
        mixed = attention_forward(qkv).reshape(rows, WIDTH)
        g_out = tie(d_out.reshape(8, images * toks, WIDTH), h_one, wqkv)
        g_out = lax.all_to_all(g_out, tp, 0, 0).reshape(rows, WIDTH)
        attn_out = dot_nn(mixed, wo_all)
        x_mid = (x_f32 + attn_out + b_o).astype(BF16)
        mid_f32 = x_mid.astype(F32)
        h_two_f, ln2_pull = jax.vjp(layer_norm, mid_f32, ln2_gain, ln2_bias)
        h_two = h_two_f.astype(BF16)
        w1_all = swap_weights(tie(w1_own_rows, h_two))
        blocks = (2, CHIPS, HALF, WIDTH)
        hidden, gelu_pulls = [], []
        for w1, b1 in zip(w1_all, b1_all):
            pre_act = dot_nt(tie(h_two, *hidden), w1)
            pre_act = (pre_act + b1).astype(BF16)
            hid_f, gelu_pull = jax.vjp(gelu_tanh, pre_act.astype(F32))
            hidden.append(hid_f.astype(BF16))
            gelu_pulls.append(gelu_pull)
        w2_oth = dot_tn(hidden[1], g_out).reshape(blocks)
        w2_got = core_swap(w2_oth)
        w2_own = dot_tn(tie(hidden[0], w2_oth), g_out).reshape(blocks)
        w2_all = swap_weights(tie(w2_own_rows, w2_own))
        w2_blk = chip_sums(w2_own, w2_got, 1)
        w2_send, w2_in = stage2(w2_blk)
        g_mlp = tie(g_out, *w2_send)
        d_pre = [None, None]
        for c in (0, 1):
            d_hidden = dot_nt(tie(g_mlp, *d_pre[:c]), w2_all[c]).astype(BF16)
            (d_pre_f,) = gelu_pulls[c](d_hidden.astype(F32))
            d_pre[c] = d_pre_f.astype(BF16)
        w1_oth = dot_tn(d_pre[1], h_two).reshape(blocks)
        w1_got = core_swap(w1_oth)
        w1_own = dot_tn(tie(d_pre[0], w1_oth), h_two).reshape(blocks)
        w1_blk = chip_sums(w1_own, w1_got, 1)
        w1_send, w1_in = stage2(w1_blk)
        d_pre_t = [tie(d, *w1_send) for d in d_pre]
        d_h_two = (dot_nn(d_pre_t[0], w1_all[0]) + dot_nn(d_pre_t[1], w1_all[1])).astype(BF16)
        d_mid_ln, g_ln2_gain, g_ln2_bias = ln2_pull(d_h_two.astype(F32))
        d_mid = (g_out.astype(F32) + d_mid_ln).astype(BF16)
        d_mixed = dot_nt(d_mid, wo_all).astype(BF16)
        dw_o = dot_tn(mixed, d_mid).reshape(CHIPS, 2, QROWS, WIDTH)
        wo_own, wo_oth = pick(dw_o, core, 1), pick(dw_o, 1 - core, 1)
        wo_got = core_swap(wo_oth)
        w2_last, w2_part = stage3(w2_blk, w2_in[0])
        d_mixed = tie(d_mixed, w2_last).reshape(8, images, toks, WIDTH)
        d_qkv = attention_backward(qkv, d_mixed).reshape(rows, 3 * WIDTH)
        w1_last, w1_part = stage3(w1_blk, w1_in[0])
        d_qkv = tie(d_qkv, w1_last)
        wo_blk = chip_sums(wo_own, wo_got, 0)
        wo_send, wo_in = stage2(wo_blk)
        dw_qkv, d_h_one, qkv_sums = projection_backward(tie(d_qkv, *wo_send), h_one, wqkv)
        dw_qkv = dw_qkv.reshape(3, CHIPS, 2, QROWS, WIDTH)
        qkv_own, qkv_oth = pick(dw_qkv, core, 2), pick(dw_qkv, 1 - core, 2)
        qkv_got = core_swap(qkv_oth)
        grad_w2 = finish(w2_blk, w2_in[1], w2_part)
        grad_w2 = grad_w2.reshape(MLP_PAD, WIDTH)[:MLP].astype(BF16)
        qkv_blk = chip_sums(qkv_own, tie(qkv_got, grad_w2), 1)
        qkv_far = lax.optimization_barrier(qkv_blk(away(1 - me)))
        far_in = permute(qkv_far, first)
        d_h_one = tie(d_h_one, qkv_oth, qkv_far)
        d_in_ln, g_ln1_gain, g_ln1_bias = ln1_pull(d_h_one.astype(F32))
        g_x = (d_mid.astype(F32) + d_in_ln).astype(BF16)
        col_sum = lambda v: jnp.sum(v, axis=0, dtype=F32)
        vecs = jnp.stack([g_ln1_gain, g_ln1_bias, col_sum(d_mid), g_ln2_gain, g_ln2_bias, col_sum(g_out)])
        head_sums = qkv_sums.reshape(3, CHIPS, 2, QROWS)
        mlp_sums = [jnp.transpose(col_sum(d).reshape(2, CHIPS, HALF), (1, 0, 2)).reshape(CHIPS, MLP_PAD) for d in d_pre]
        mlp_sums = jnp.where(core0, jnp.stack(mlp_sums, 1), jnp.stack(mlp_sums[::-1], 1))
        bias_sums = jnp.concatenate([head_sums[0], head_sums[2], mlp_sums, jnp.zeros((CHIPS, 2, WIDTH - 2 * QROWS - MLP_PAD), F32)], axis=2)
        small = jnp.concatenate([jnp.broadcast_to(vecs, (CHIPS, 6, WIDTH)), bias_sums], axis=1)
        small_send = lax.optimization_barrier(jnp.stack([pick(small, away(me)), pick(small, away(1 - me))]))
        small_in = permute(small_send, first)
        near_send = lax.optimization_barrier(qkv_blk(away(me)))
        near_in = permute(near_send, first)
        grad_x = lax.all_to_all(g_x.reshape(8, images * toks, WIDTH), tp, 0, 0).reshape(x.shape)
        _, wo_part = stage3(wo_blk, wo_in[0])
        mlp_out = dot_nn(tie(hidden[0], near_send, g_x), w2_all[0])
        mlp_out = mlp_out + dot_nn(hidden[1], w2_all[1])
        y_rows = (mid_f32 + mlp_out + b_2).astype(BF16)
        y_out = lax.all_to_all(tie(y_rows, grad_x).reshape(8, images * toks, WIDTH), tp, 0, 0).reshape(x.shape)
        qkv_last, qkv_part = stage3(qkv_blk, tie(far_in, near_send))
        grad_w1 = finish(w1_blk, w1_in[1], tie(w1_part, qkv_last))
        grad_w1 = grad_w1.reshape(MLP_PAD, WIDTH)[:MLP].T.astype(BF16)
        near_in = tie(near_in, qkv_last, grad_w1)
        small_far = pick(small, near(1 - me)) + small_in[1]
        small_part = permute(small_far, second)
        grad_qkv = finish(qkv_blk, near_in, qkv_part).astype(BF16)
        small_own = pick(small, near(me)) + small_in[0] + small_part
        extra = small_own + core_swap(small_own)
        b_row = pick(extra[6:], core).astype(BF16)

        grad_wo = finish(wo_blk, wo_in[1], tie(wo_part, qkv_last))
        grad_wo = grad_wo.reshape(HEADS, HEAD_DIM, WIDTH).astype(BF16)
        unrow = lambda w: jnp.transpose(w.reshape(HEADS, HEAD_DIM, WIDTH), (2, 0, 1))

        return (y_out, grad_x, extra[0], extra[1], unrow(grad_qkv[0]), b_row[:QROWS].reshape(HEADS, HEAD_DIM),
                unrow(grad_qkv[1]), unrow(grad_qkv[2]), b_row[QROWS:2 * QROWS].reshape(HEADS, HEAD_DIM), grad_wo,
                extra[2].astype(BF16), extra[3], extra[4], grad_w1, b_row[2 * QROWS:2 * QROWS + MLP], grad_w2,
                extra[5].astype(BF16))

    return jax.shard_map(layer_step, mesh=mesh3, in_specs=in_specs, out_specs=out_specs, check_vma=False)
```
